256 devices in a mesh: row: 32 (over y, z_lo, x), col: 8 (over z_hi, core).
Axes of the slice: x: 4, y: 4, z: 8 (z_hi: 4, z_lo: 2; z = z_hi * 2 + z_lo), core: 2. Of those that a mesh axis runs over, the one named last changes fastest.
Arguments:
- noise: bfloat16 [8, 2, 32, 2048], P(None, None, 'row', 'col'), may hold values from -6 to 6
- diag_factor: bfloat16 [2, 32, 2048, 2048], P(None, 'row', 'col'), may hold values from -0.125 to 0.125
- left_factor: bfloat16 [32, 64, 64, 2048], P('row', None, None, 'col'), may hold values from -0.09375 to 0.09375
- right_factor: bfloat16 [32, 64, 64, 2048], P('row', None, None, 'col'), may hold values from -0.125 to 0.125
- tile_ranks: int32 [32, 64], P('row'), may hold values from 1 to 64
- pair_first: int32 [32, 8, 4096], P('row', 'col'), may hold values from 4096 to 8191
- pair_partner: int32 [32, 8, 4096], P('row', 'col'), may hold values from 0 to 8191, as said below
- bin_ids: int32 [32, 8, 4096], P('row', 'col'), may hold values from 0 to 127, as said below
Outputs:
- samples: float32 [8, 2, 32, 2048], P(None, None, 'row', 'col')
- variogram: float32 [8, 128], replicated
The draws below stay inside these ranges and needn't reach their ends.
Inputs may be any that keep to these rules, and one draw needn't show every extreme that they name: Pairs of the first tile-row pair (r = 0) have pair_partner of 4096 or more. `bin_ids`: bins may hold no pair.
All inputs are finite; a program needn't handle non-finite values.
Results may differ from the reference program's by a relative error of at most 0.0012.
Values may be sent and summed in bfloat16 or wider, within the bound.
No kernel may reach another device: no remote copies, remote signals or barrier semaphores. Data moves between devices by JAX's collectives and lax.ppermute only.
A program may use at most 64 MiB of HBM per device.

```python
import jax
import jax.numpy as jnp
from jax import lax

SAMPLES = 8
TILE = 2048
RMAX = 64
NBIN = 128
PAIRS = 4096
NT = 64
N_ROW = 32
N_COL = 8


def draw_pair_partner(key, part):
    first_row = jnp.arange(N_ROW, dtype=jnp.int32) == 0
    lowest = jnp.where(first_row, 2 * TILE, 0).astype(jnp.int32)[:, None, None]
    return jax.random.randint(key, (N_ROW, N_COL, PAIRS), lowest, 4 * TILE, dtype=jnp.int32)


def draw_bin_ids(key, part):
    order_key = jax.random.fold_in(key, 101)
    choose_key = jax.random.fold_in(key, 202)
    bin_order = jax.random.permutation(order_key, NBIN).astype(jnp.int32)
    live_count = NBIN - max(1, NBIN // 8)
    pick_index = jax.random.randint(choose_key, (N_ROW, N_COL, PAIRS), 0, live_count, dtype=jnp.int32)
    return jnp.take(bin_order, pick_index).astype(jnp.int32)


def set_ends(drawn, own_key, least, largest):
    extent = drawn.shape
    spot = [jax.random.randint(jax.random.fold_in(own_key, axis), (), 0, extent[axis]) for axis in range(len(extent))]
    drawn = drawn.at[tuple(spot)].set(least)
    longest = extent.index(max(extent))
    spot[longest] = (spot[longest] + 1) % extent[longest]
    return drawn.at[tuple(spot)].set(largest)


def block_scale(rng, extent, split, smallest, largest):
    def one(position, parts):
        heights = jax.random.uniform(jax.random.fold_in(jax.random.fold_in(rng, 6), position), (parts,), jnp.float32, smallest / len(split), largest / len(split))
        return jnp.repeat(jnp.exp(heights), extent[position] // parts).reshape((-1,) + (1,) * (len(extent) - position - 1))

    level = one(*split[0])
    for cut in split[1:]:
        level = level * one(*cut)
    return level


def normal_values(rng, extent, spread, limit, pieces=(), kind=jnp.bfloat16):
    factor_of = block_scale(rng, extent, pieces, -0.22, 0.18) if pieces else 1.0
    array = jax.random.normal(rng, extent, jnp.float32) * spread * factor_of
    return jnp.minimum(jnp.maximum(array, -limit), limit).astype(kind)


def setup_inputs(seed: int = 0) -> dict:
    key_of = jax.random.split(jax.random.key(seed), 9)
    return {
        "noise": normal_values(key_of[0], (SAMPLES, 2, N_ROW, TILE), 1.0, 6.0, ((2, 32), (3, 8))),
        "diag_factor": normal_values(key_of[1], (2, N_ROW, TILE, TILE), TILE ** -0.5, 0.125, ((1, 32), (2, 8))),
        "left_factor": normal_values(key_of[2], (N_ROW, NT, RMAX, TILE), (RMAX * NT) ** -0.5, 0.09375, ((0, 32), (3, 8))),
        "right_factor": normal_values(key_of[3], (N_ROW, NT, RMAX, TILE), TILE ** -0.5, 0.125, ((0, 32), (3, 8))),
        "tile_ranks": set_ends(jax.random.randint(key_of[4], (N_ROW, NT), 1, RMAX + 1), jax.random.fold_in(key_of[4], 1), 1, RMAX).astype(jnp.int32),
        "pair_first": set_ends(jax.random.randint(key_of[5], (N_ROW, N_COL, PAIRS), 2 * TILE, 4 * TILE), jax.random.fold_in(key_of[5], 1), 2 * TILE, (4 * TILE) - 1).astype(jnp.int32),
        "pair_partner": draw_pair_partner(jax.random.fold_in(key_of[8], 71), 0),
        "bin_ids": draw_bin_ids(jax.random.fold_in(key_of[8], 71), 0),
    }


def reference(noise, diag_factor, left_factor, right_factor, tile_ranks, pair_first, pair_partner, bin_ids):
    tile_count = 2 * N_ROW
    ordered = jnp.concatenate([noise[:, 0], noise[:, 1][:, ::-1]], axis=1)
    idx_tile = jnp.arange(TILE, dtype=jnp.int32)
    below = idx_tile[None, :] < idx_tile[:, None]
    ident = (idx_tile[None, :] == idx_tile[:, None]).astype(jnp.float32)
    slot_ids = jnp.arange(tile_count, dtype=jnp.int32)
    rank_ids = jnp.arange(RMAX, dtype=jnp.int32)

    def one_pair(pair_id):
        tiles_diag = diag_factor[:, pair_id].astype(jnp.float32)
        effective = jnp.where(below[None], tiles_diag, 0.0) + ident[None]
        own_noise = jnp.stack([ordered[:, pair_id], ordered[:, tile_count - 1 - pair_id]], axis=1).astype(jnp.float32)
        on_diag = jnp.einsum('sht,hit->shi', own_noise, effective, precision=lax.Precision.HIGHEST)
        source = jnp.where(slot_ids < pair_id, slot_ids, slot_ids - pair_id).astype(jnp.int32)
        chosen = jnp.take(ordered, source, axis=1).astype(jnp.float32)
        projected = jnp.einsum('skt,kqt->ksq', chosen, right_factor[pair_id].astype(jnp.float32), precision=lax.Precision.HIGHEST)
        in_rank = rank_ids[None, :] < tile_ranks[pair_id][:, None]
        coeffs = jnp.where(in_rank[:, None, :], projected, 0.0).astype(jnp.bfloat16)
        coeffs = lax.optimization_barrier(coeffs).astype(jnp.float32)
        select = jnp.stack([slot_ids < pair_id, (slot_ids >= pair_id) & (slot_ids < tile_count - 1)]).astype(jnp.float32)
        weighted = select[:, :, None, None] * coeffs[None]
        off_diag = jnp.einsum('hksq,kqt->sht', weighted, left_factor[pair_id].astype(jnp.float32), precision=lax.Precision.HIGHEST)
        return on_diag + off_diag

    stacked = lax.map(one_pair, jnp.arange(N_ROW, dtype=jnp.int32))
    samples = jnp.transpose(stacked, (1, 2, 0, 3))
    previous = jnp.concatenate([jnp.zeros_like(samples[:, :, :1]), samples[:, :, :-1]], axis=2)
    pooled = jnp.concatenate([previous[:, 0], previous[:, 1], samples[:, 0], samples[:, 1]], axis=-1)
    first_idx = pair_first.reshape(N_ROW, N_COL * PAIRS)
    second_idx = pair_partner.reshape(N_ROW, N_COL * PAIRS)
    first_val = jnp.take_along_axis(pooled, first_idx[None], axis=2)
    second_val = jnp.take_along_axis(pooled, second_idx[None], axis=2)
    differ = first_val - second_val
    half_sq = 0.5 * differ * differ
    half_sq = jnp.transpose(half_sq.reshape(SAMPLES, N_ROW * N_COL, PAIRS), (1, 0, 2))
    bin_blocks = bin_ids.reshape(N_ROW * N_COL, PAIRS)
    bin_range = jnp.arange(NBIN, dtype=jnp.int32)

    def add_block(carry, items):
        block_sq, block_bins = items
        onehot = (block_bins[:, None] == bin_range[None, :]).astype(jnp.float32)
        sums = carry[0] + jnp.dot(block_sq, onehot, precision=lax.Precision.HIGHEST, preferred_element_type=jnp.float32)
        counts = carry[1] + jnp.sum(onehot, axis=0)
        return (sums, counts), None

    start = (jnp.zeros((SAMPLES, NBIN), jnp.float32), jnp.zeros((NBIN,), jnp.float32))
    (bin_sums, bin_counts), _ = lax.scan(add_block, start, (half_sq, bin_blocks))
    variogram = bin_sums / jnp.maximum(bin_counts, 1.0)[None, :]
    return samples, variogram
```

```python
import functools

import jax
import jax.numpy as jnp
from jax import lax
from jax.experimental import pallas as pl
from jax.experimental.pallas import tpu as pltpu
from jax.sharding import Mesh
from jax.sharding import PartitionSpec as P

NBIN = 128
ROW = ("row_0", "row_1", "row_2")
COL = ("col_0", "col_1")
XY = ("row_0", "row_2")
ZC = ("row_1", "col_0", "col_1")
F32 = jnp.float32
BF16 = jnp.bfloat16


def exchange(copies, axis):
    return lax.all_to_all(copies, axis, 0, 0, tiled=True)


def copies_of(x, axis):
    return jnp.broadcast_to(x[None], (lax.axis_size(axis), *x.shape))


def nt_dot(a, b):
    return lax.dot_general(a, b, (((1,), (1,)), ((), ())), preferred_element_type=F32)


def call(kernel, out_shape, in_specs, flops=1, **kw):
    return pl.pallas_call(
        kernel,
        out_shape=out_shape,
        in_specs=in_specs,
        cost_estimate=pl.CostEstimate(flops=flops, bytes_accessed=1 << 20, transcendentals=0),
        **kw,
    )


VM = pl.BlockSpec(memory_space=pltpu.VMEM)
SM = pl.BlockSpec(memory_space=pltpu.SMEM)


def project_kernel(place, columns, right, keep, send):
    row, core = place[0], place[1]
    tiles = 2 * columns.shape[0]
    groups = right.shape[0] // 8
    lane = lax.broadcasted_iota(jnp.int32, (8, 128), 1)
    for half, out in ((core, keep), (1 - core, send)):
        def step(g, carry, half=half, out=out):
            base = (half * groups + g) * 4
            blocks = []
            low = []
            for n in range(4):
                slot = base + n
                tile = jnp.where(slot < row, slot, slot - row)
                first = tile < tiles // 2
                blocks.append(columns[jnp.where(first, tile, tiles - 1 - tile)])
                low.append(first)
            factor = right[pl.ds(base, 4)].reshape(256, 256)
            full = nt_dot(jnp.concatenate(blocks, axis=0), factor)
            parts = []
            for n in range(4):
                cols = full[16 * n : 16 * n + 16, 128 * (n // 2) : 128 * (n // 2) + 128]
                parts.append(jnp.where(low[n], cols[:8], cols[8:]))
            out[2 * g] = jnp.where(lane < 64, parts[0], parts[1])
            out[2 * g + 1] = jnp.where(lane < 64, parts[2], parts[3])
            return carry
        lax.fori_loop(0, groups, step, 0, unroll=4)


def coeff_kernel(place, ranks, sums, out):
    core = place[1]
    lane = lax.broadcasted_iota(jnp.int32, (8, 128), 1)
    left = lane < 64
    blocks = sums.shape[1]
    for i in range(blocks):
        slot = 2 * (core * blocks + i)
        total = sums[0, i] + sums[1, i] + sums[2, i] + sums[3, i]
        limit = jnp.where(left, ranks[0, slot], ranks[0, slot + 1] + 64)
        out[i] = jnp.where(lane < limit, total, 0.0).astype(BF16)


def on_diag_kernel(place, noise, diag, out):
    col = place[2]
    span = noise.shape[2]
    i_at = lax.broadcasted_iota(jnp.int32, (span, span), 0)
    j_at = lax.broadcasted_iota(jnp.int32, (span, span), 1)
    gap = j_at - i_at
    own = noise[col].astype(F32)
    acc = [own[:8], own[8:]]
    for piece in range(noise.shape[0]):
        below = gap < (col - piece) * span
        for h in range(2):
            tile = diag[h, :, piece * span : (piece + 1) * span]
            tile = jnp.where(below, tile.astype(F32), 0.0).astype(BF16)
            acc[h] = acc[h] + nt_dot(noise[piece], tile)[8 * h : 8 * h + 8]
    out[...] = jnp.concatenate(acc, axis=0)


def sample_kernel(place, mine, theirs, left, on_diag, out):
    row, core = place[0], place[1]
    blocks = mine.shape[0]
    last = 4 * blocks - 1
    lane = lax.broadcasted_iota(jnp.int32, (8, 128), 1)
    side = jnp.where(lane < 64, 0, 1)
    acc = on_diag[...]
    for half, coeffs in ((core, mine), (1 - core, theirs)):
        rows = []
        for i in range(blocks):
            slot = 2 * (half * blocks + i) + side
            c = coeffs[i].astype(F32)
            upper = jnp.where(slot < row, c, 0.0)
            lower = jnp.where((slot >= row) & (slot < last), c, 0.0)
            rows.append(jnp.concatenate([upper, lower], axis=0).astype(BF16))
        weights = jnp.concatenate(rows, axis=1)
        factor = left[pl.ds(half * blocks, blocks)].reshape(blocks * 128, left.shape[2])
        acc = acc + jnp.dot(weights, factor, preferred_element_type=F32)
    for n in range(out.shape[0]):
        out[n] = acc


def lookup(table, idx):
    low = idx & 127
    bit = [((idx >> (7 + n)) & 1) == 1 for n in range(5)]

    def tree(level, number):
        if level < 0:
            h, piece, half = number >> 4, (number >> 1) & 7, number & 1
            source = table[piece, 8 * h : 8 * h + 8, 128 * half : 128 * half + 128]
            return jnp.take_along_axis(source, low, axis=1, mode="promise_in_bounds")
        zero = tree(level - 1, number)
        one = tree(level - 1, number | (1 << level))
        return jnp.where(bit[level], one, zero)

    return tree(4, 0)


def own_kernel(table, first, partner, out):
    def step(n, carry):
        at = pl.multiple_of(n * 128, 128)
        a = jnp.broadcast_to(first[:, pl.ds(at, 128)], (8, 128))
        b = jnp.broadcast_to(partner[:, pl.ds(at, 128)], (8, 128))
        other = jnp.where(b >= 4096, lookup(table, b), 0.0)
        out[:, pl.ds(at, 128)] = lookup(table, a) - other
        return carry

    lax.fori_loop(0, first.shape[1] // 128, step, 0)


def bin_kernel(prev, partner, base, bins, out, table, pieces, onehot):
    table[...] = prev[...].astype(F32)
    bin_at = lax.broadcasted_iota(jnp.int32, (NBIN, 128), 0)

    def step(n, carry):
        at = pl.multiple_of(n * 128, 128)
        b = jnp.broadcast_to(partner[:, pl.ds(at, 128)], (8, 128))
        differ = base[:, pl.ds(at, 128)] - jnp.where(b < 4096, lookup(table, b), 0.0)
        value = 0.5 * differ * differ
        top = value.astype(BF16).astype(F32)
        rest = value - top
        mid = rest.astype(BF16).astype(F32)
        stack = jnp.concatenate([top, mid, rest - mid, jnp.ones_like(value)], axis=0)
        pieces[:, pl.ds(at, 128)] = stack.astype(BF16)
        ids = jnp.broadcast_to(bins[:, pl.ds(at, 128)], (NBIN, 128))
        onehot[:, pl.ds(at, 128)] = jnp.where(ids == bin_at, 1.0, 0.0).astype(BF16)
        return carry

    lax.fori_loop(0, partner.shape[1] // 128, step, 0)
    total = nt_dot(pieces[...], onehot[...])
    sums = (total[:8] + total[8:16]) + total[16:24]
    result = jnp.concatenate([sums, total[24:]], axis=0)
    for n in range(out.shape[0]):
        out[n] = result


def merge_kernel(parts, out):
    total = parts[0]
    for n in range(1, parts.shape[0]):
        total = total + parts[n]
    for n in range(out.shape[0]):
        out[n] = total


def finish_kernel(parts, out):
    total = parts[0]
    for n in range(1, parts.shape[0]):
        total = total + parts[n]
    out[...] = total[:8] / jnp.maximum(total[8:], 1.0)


def sds(shape, dtype):
    return jax.ShapeDtypeStruct(shape, dtype)


def body(
    noise, diag_factor, left_factor, right_factor, tile_ranks, pair_first, pair_partner, bin_ids
):
    row_at = lax.axis_index(ROW)
    col_at = lax.axis_index(COL)
    core_at = lax.axis_index("col_1")
    rows = lax.axis_size(ROW)
    cols = lax.axis_size(COL)
    place = jnp.stack([row_at, core_at, col_at]).astype(jnp.int32)
    span = noise.shape[3]
    swap = [(0, 1), (1, 0)]

    local = jnp.transpose(noise[:, :, 0], (1, 0, 2)).reshape(16, span)
    columns = exchange(copies_of(local, ROW), ROW)
    own_noise = exchange(copies_of(local, COL), COL)

    keep, send = call(
        project_kernel,
        (sds((16, 8, 128), F32), sds((16, 8, 128), F32)),
        [SM, VM, VM],
        flops=1 << 28,
        name="project",
    )(place, columns, right_factor[0])
    received = lax.ppermute(send, "col_1", swap)
    sums = exchange(copies_of(keep + received, "col_0"), "col_0")
    on_diag = call(on_diag_kernel, sds((16, span), F32), [SM, VM, VM], flops=1 << 28, name="ondiag")(
        place, own_noise, diag_factor[:, 0]
    )
    mine = call(coeff_kernel, sds((16, 8, 128), BF16), [SM, SM, VM], name="coeffs")(
        place, tile_ranks, sums
    )
    theirs = lax.ppermute(mine, "col_1", swap)
    copies = call(
        sample_kernel,
        sds((cols, 16, span), F32),
        [SM, VM, VM, VM, VM],
        flops=1 << 26,
        name="samples",
    )(place, mine, theirs, left_factor[0].reshape(32, 128, span), on_diag)
    samples = jnp.transpose(copies[0].reshape(2, 8, span), (1, 0, 2))[:, :, None]

    own_tiles = exchange(copies, COL)
    prev_tiles = lax.ppermute(
        own_tiles.astype(BF16), ROW, [(source, source + 1) for source in range(rows - 1)]
    )
    first, partner, bins = pair_first[0], pair_partner[0], bin_ids[0]
    pairs = first.shape[1]
    base = call(own_kernel, sds((8, pairs), F32), [VM, VM, VM], flops=1 << 26, name="own")(
        own_tiles, first, partner
    )
    partial = call(
        bin_kernel,
        sds((lax.axis_size(ZC), 16, NBIN), F32),
        [VM, VM, VM, VM],
        flops=1 << 26,
        scratch_shapes=[
            pltpu.VMEM((cols, 16, span), F32),
            pltpu.VMEM((32, pairs), BF16),
            pltpu.VMEM((NBIN, pairs), BF16),
        ],
        name="bins",
    )(prev_tiles, partner, base, bins)
    merged = call(merge_kernel, sds((lax.axis_size(XY), 16, NBIN), F32), [VM], name="merge")(
        exchange(partial, ZC)
    )
    variogram = call(finish_kernel, sds((8, NBIN), F32), [VM], name="finish")(exchange(merged, XY))
    return (samples, variogram)


def solution(mesh):
    split = Mesh(mesh.devices.reshape(4, 2, 4, 4, 2), ("row_0", "row_1", "row_2", "col_0", "col_1"))
    return jax.shard_map(
        body,
        mesh=split,
        in_specs=(
            P(None, None, ROW, COL),
            P(None, ROW, COL, None),
            P(ROW, None, None, COL),
            P(ROW, None, None, COL),
            P(ROW, None),
            P(ROW, COL, None),
            P(ROW, COL, None),
            P(ROW, COL, None),
        ),
        out_specs=(P(None, None, ROW, COL), P()),
        check_vma=False,
    )
```

```python
import jax
import jax.numpy as jnp
from jax import lax
from jax.experimental import pallas as pl
from jax.experimental.pallas import tpu as pltpu
from jax.sharding import Mesh
from jax.sharding import PartitionSpec as P

NBIN = 128
ROW = ("row_0", "row_1", "row_2")
COL = ("col_0", "col_1")
XY = ("row_0", "row_2")
ZC = ("row_1", "col_0", "col_1")
F32 = jnp.float32
BF16 = jnp.bfloat16


def exchange(copies, axis):
    return lax.all_to_all(copies, axis, 0, 0, tiled=True)


def copies_of(x, axis):
    return jnp.broadcast_to(x[None], (lax.axis_size(axis), *x.shape))


def nt_dot(a, b):
    return lax.dot_general(a, b, (((1,), (1,)), ((), ())), preferred_element_type=F32)


HB = pl.BlockSpec(memory_space=pltpu.HBM)
VM = pl.BlockSpec(memory_space=pltpu.VMEM)
SM = pl.BlockSpec(memory_space=pltpu.SMEM)


def call(kernel, out_shape, in_specs, flops=1, **kw):
    run = pl.pallas_call(
        kernel,
        out_shape=out_shape,
        in_specs=in_specs,
        cost_estimate=pl.CostEstimate(flops=flops, bytes_accessed=1 << 20, transcendentals=0),
        compiler_params=pltpu.CompilerParams(vmem_limit_bytes=16 << 20),
        **kw,
    )

    def held(*args):
        return run(
            *(
                a if spec is SM else pltpu.with_memory_space_constraint(a, spec.memory_space)
                for a, spec in zip(args, in_specs)
            )
        )

    return held


def stage_kernel(source, out, sem):
    copy = pltpu.make_async_copy(source, out, sem)
    copy.start()
    copy.wait()


def spread_kernel(place, keep, received, noise, other, out):
    blocks = keep.shape[0]
    first = place[1] == 0
    own = noise[...].astype(F32)
    far = other[...].astype(F32)
    pieces = (jnp.where(first, own, far).astype(BF16), jnp.where(first, far, own).astype(BF16))
    copies = out.shape[0]
    for i in range(0, blocks, 2):
        total = jnp.concatenate([keep[i] + received[i], keep[i + 1] + received[i + 1]], axis=0)
        top = total.astype(BF16)
        rest = (total - top.astype(F32)).astype(BF16)
        for n in range(copies):
            out[n, 8 * i : 8 * i + 16] = top
            out[n, 8 * (blocks + i) : 8 * (blocks + i) + 16] = rest
    for core in range(2):
        for side in range(2):
            at = 16 * (blocks + 2 * core + side)
            for n in range(copies):
                out[n, at : at + 16] = pieces[core][:, 128 * side : 128 * side + 128]


def project_kernel(place, columns, right, keep, send):
    row, core = place[0], place[1]
    tiles = 2 * columns.shape[0]
    groups = right.shape[0] // 8
    lane = lax.broadcasted_iota(jnp.int32, (8, 128), 1)
    for half, out in ((core, keep), (1 - core, send)):
        def step(g, carry, half=half, out=out):
            base = (half * groups + g) * 4
            blocks = []
            low = []
            for n in range(4):
                slot = base + n
                tile = jnp.where(slot < row, slot, slot - row)
                first = tile < tiles // 2
                blocks.append(columns[jnp.where(first, tile, tiles - 1 - tile)])
                low.append(first)
            factor = right[pl.ds(base, 4)].reshape(256, 256)
            full = nt_dot(jnp.concatenate(blocks, axis=0), factor)
            parts = []
            for n in range(4):
                cols = full[16 * n : 16 * n + 16, 128 * (n // 2) : 128 * (n // 2) + 128]
                parts.append(jnp.where(low[n], cols[:8], cols[8:]))
            out[2 * g] = jnp.where(lane < 64, parts[0], parts[1])
            out[2 * g + 1] = jnp.where(lane < 64, parts[2], parts[3])
            return carry

        lax.fori_loop(0, groups, step, 0, unroll=4)


def coeff_kernel(place, ranks, parts, out):
    core = place[1]
    lane = lax.broadcasted_iota(jnp.int32, (8, 128), 1)
    left = lane < 64
    blocks = out.shape[0]
    for i in range(0, blocks, 2):
        total = jnp.zeros((16, 128), F32)
        for n in range(parts.shape[0]):
            top = parts[n, 8 * i : 8 * i + 16].astype(F32)
            total = total + (top + parts[n, 8 * (blocks + i) : 8 * (blocks + i) + 16].astype(F32))
        for k in range(2):
            slot = 2 * (core * blocks + i + k)
            limit = jnp.where(left, ranks[0, slot], ranks[0, slot + 1] + 64)
            out[i + k] = jnp.where(lane < limit, total[8 * k : 8 * k + 8], 0.0).astype(BF16)


def on_diag_kernel(place, parts, diag, out):
    col = place[2]
    span = diag.shape[1]
    pieces = []
    own = jnp.zeros((16, span), F32)
    for n in range(parts.shape[0]):
        for core in range(2):
            at = 256 + 32 * core
            piece = jnp.concatenate([parts[n, at : at + 16], parts[n, at + 16 : at + 32]], axis=1)
            piece = piece.astype(F32)
            number = 2 * n + core
            own = jnp.where(col == number, piece, own)
            pieces.append(jnp.where(number < col, piece, 0.0).astype(BF16))
    before = jnp.concatenate(pieces, axis=1)
    i_at = lax.broadcasted_iota(jnp.int32, (span, span), 0)
    j_at = lax.broadcasted_iota(jnp.int32, (span, span), 1)
    at = pl.multiple_of(col * span, span)
    for h in range(2):
        corner = jnp.where(j_at < i_at, diag[h, :, pl.ds(at, span)].astype(F32), 0.0).astype(BF16)
        total = nt_dot(before, diag[h]) + nt_dot(own.astype(BF16), corner) + own
        out[8 * h : 8 * h + 8] = total[8 * h : 8 * h + 8]


def sample_kernel(place, mine, theirs, left, on_diag, out):
    row, core = place[0], place[1]
    blocks = mine.shape[0]
    last = 4 * blocks - 1
    lane = lax.broadcasted_iota(jnp.int32, (8, 128), 1)
    side = jnp.where(lane < 64, 0, 1)
    acc = on_diag[...]
    for half, coeffs in ((core, mine), (1 - core, theirs)):
        rows = []
        for i in range(blocks):
            slot = 2 * (half * blocks + i) + side
            c = coeffs[i].astype(F32)
            upper = jnp.where(slot < row, c, 0.0)
            lower = jnp.where((slot >= row) & (slot < last), c, 0.0)
            rows.append(jnp.concatenate([upper, lower], axis=0).astype(BF16))
        weights = jnp.concatenate(rows, axis=1)
        factor = left[pl.ds(half * blocks, blocks)].reshape(blocks * 128, left.shape[2])
        acc = acc + jnp.dot(weights, factor, preferred_element_type=F32)
    for n in range(out.shape[0]):
        out[n] = acc


def lookup(table, idx):
    low = idx & 127
    bit = [((idx >> (7 + n)) & 1) == 1 for n in range(5)]

    def tree(level, number):
        if level < 0:
            h, piece, half = number >> 4, (number >> 1) & 7, number & 1
            source = table[piece, 8 * h : 8 * h + 8, 128 * half : 128 * half + 128]
            return jnp.take_along_axis(source, low, axis=1, mode="promise_in_bounds")
        zero = tree(level - 1, number)
        one = tree(level - 1, number | (1 << level))
        return jnp.where(bit[level], one, zero)

    return tree(4, 0)


def own_kernel(table, first, partner, out):
    def step(n, carry):
        at = pl.multiple_of(n * 128, 128)
        a = jnp.broadcast_to(first[:, pl.ds(at, 128)], (8, 128))
        b = jnp.broadcast_to(partner[:, pl.ds(at, 128)], (8, 128))
        other = jnp.where(b >= 4096, lookup(table, b), 0.0)
        out[:, pl.ds(at, 128)] = lookup(table, a) - other
        return carry

    lax.fori_loop(0, first.shape[1] // 128, step, 0, unroll=4)


def bin_kernel(prev, partner, base, bins, out, table, pieces, onehot):
    table[...] = prev[...].astype(F32)
    bin_at = lax.broadcasted_iota(jnp.int32, (NBIN, 128), 0)

    def step(n, carry):
        at = pl.multiple_of(n * 128, 128)
        b = jnp.broadcast_to(partner[:, pl.ds(at, 128)], (8, 128))
        differ = base[:, pl.ds(at, 128)] - jnp.where(b < 4096, lookup(table, b), 0.0)
        value = 0.5 * differ * differ
        top = value.astype(BF16).astype(F32)
        rest = value - top
        mid = rest.astype(BF16).astype(F32)
        stack = jnp.concatenate([top, mid, rest - mid, jnp.ones_like(value)], axis=0)
        pieces[:, pl.ds(at, 128)] = stack.astype(BF16)
        ids = jnp.broadcast_to(bins[:, pl.ds(at, 128)], (NBIN, 128))
        onehot[:, pl.ds(at, 128)] = jnp.where(ids == bin_at, 1.0, 0.0).astype(BF16)
        return carry

    lax.fori_loop(0, partner.shape[1] // 128, step, 0, unroll=4)
    total = nt_dot(pieces[...], onehot[...])
    sums = (total[:8] + total[8:16]) + total[16:24]
    result = jnp.concatenate([sums, total[24:]], axis=0)
    for n in range(out.shape[0]):
        out[n] = result


def merge_kernel(parts, out):
    total = parts[0]
    for n in range(1, parts.shape[0]):
        total = total + parts[n]
    for n in range(out.shape[0]):
        out[n] = total


def finish_kernel(parts, out):
    total = parts[0]
    for n in range(1, parts.shape[0]):
        total = total + parts[n]
    out[...] = total[:8] / jnp.maximum(total[8:], 1.0)


def vmem(shape, dtype):
    return pltpu.VMEM(shape, dtype)


def body(
    noise, diag_factor, left_factor, right_factor, tile_ranks, pair_first, pair_partner, bin_ids
):
    row_at = lax.axis_index(ROW)
    col_at = lax.axis_index(COL)
    core_at = lax.axis_index("col_1")
    rows = lax.axis_size(ROW)
    cols = lax.axis_size(COL)
    place = jnp.stack([row_at, core_at, col_at]).astype(jnp.int32)
    span = noise.shape[3]
    swap = [(0, 1), (1, 0)]

    local = jnp.transpose(noise[:, :, 0], (1, 0, 2)).reshape(16, span)
    columns = exchange(copies_of(local, ROW), ROW)
    other_noise = lax.ppermute(local, "col_1", swap)
    right = call(
        stage_kernel,
        vmem(right_factor.shape[1:], BF16),
        [HB],
        scratch_shapes=[pltpu.SemaphoreType.DMA(())],
        name="stage",
    )(right_factor[0])

    keep, send = call(
        project_kernel,
        (vmem((16, 8, 128), F32), vmem((16, 8, 128), F32)),
        [SM, VM, VM],
        flops=1 << 28,
        name="project",
    )(place, columns, right)
    received = lax.ppermute(send, "col_1", swap)
    spread = call(
        spread_kernel, vmem((4, 320, 128), BF16), [SM, VM, VM, VM, VM], name="spread"
    )(place, keep, received, local, other_noise)
    sums = exchange(spread, "col_0")
    mine = call(coeff_kernel, vmem((16, 8, 128), BF16), [SM, SM, VM], name="coeffs")(
        place, tile_ranks, sums
    )
    theirs = lax.ppermute(mine, "col_1", swap)
    on_diag = call(
        on_diag_kernel, vmem((16, span), F32), [SM, VM, VM], flops=1 << 28, name="ondiag"
    )(place, sums, diag_factor[:, 0])
    copies = call(
        sample_kernel,
        vmem((cols, 16, span), F32),
        [SM, VM, VM, VM, VM],
        flops=1 << 26,
        name="samples",
    )(place, mine, theirs, left_factor[0].reshape(32, 128, span), on_diag)
    samples = jnp.transpose(copies[0].reshape(2, 8, span), (1, 0, 2))[:, :, None]

    own_tiles = exchange(copies, COL)
    prev_tiles = lax.ppermute(
        own_tiles.astype(BF16), ROW, [(source, source + 1) for source in range(rows - 1)]
    )
    first, partner, bins = pair_first[0], pair_partner[0], bin_ids[0]
    pairs = first.shape[1]
    base = call(own_kernel, vmem((8, pairs), F32), [VM, VM, VM], flops=1 << 26, name="own")(
        own_tiles, first, partner
    )
    partial = call(
        bin_kernel,
        vmem((lax.axis_size(ZC), 16, NBIN), F32),
        [VM, VM, VM, VM],
        flops=1 << 26,
        scratch_shapes=[
            pltpu.VMEM((cols, 16, span), F32),
            pltpu.VMEM((32, pairs), BF16),
            pltpu.VMEM((NBIN, pairs), BF16),
        ],
        name="bins",
    )(prev_tiles, partner, base, bins)
    merged = call(merge_kernel, vmem((lax.axis_size(XY), 16, NBIN), F32), [VM], name="merge")(
        exchange(partial, ZC)
    )
    variogram = call(finish_kernel, jax.ShapeDtypeStruct((8, NBIN), F32), [VM], name="finish")(exchange(merged, XY))
    return (samples, variogram)


def solution(mesh):
    split = Mesh(mesh.devices.reshape(4, 2, 4, 4, 2), ("row_0", "row_1", "row_2", "col_0", "col_1"))
    return jax.shard_map(
        body,
        mesh=split,
        in_specs=(
            P(None, None, ROW, COL),
            P(None, ROW, COL, None),
            P(ROW, None, None, COL),
            P(ROW, None, None, COL),
            P(ROW, None),
            P(ROW, COL, None),
            P(ROW, COL, None),
            P(ROW, COL, None),
        ),
        out_specs=(P(None, None, ROW, COL), P()),
        check_vma=False,
    )
```

```python
import jax
import jax.numpy as jnp
from jax import lax
from jax.experimental import pallas as pl
from jax.experimental.pallas import tpu as pltpu
from jax.sharding import Mesh
from jax.sharding import PartitionSpec as P

NBIN = 128
ROW = ("row_0", "row_1", "row_2")
COL = ("col_0", "col_1")
XY = ("row_0", "row_2")
ZC = ("row_1", "col_0", "col_1")
F32 = jnp.float32
BF16 = jnp.bfloat16


def exchange(copies, axis):
    return lax.all_to_all(copies, axis, 0, 0, tiled=True)


def nt_dot(a, b):
    return lax.dot_general(a, b, (((1,), (1,)), ((), ())), preferred_element_type=F32)


HB = pl.BlockSpec(memory_space=pltpu.HBM)
VM = pl.BlockSpec(memory_space=pltpu.VMEM)
SM = pl.BlockSpec(memory_space=pltpu.SMEM)


def call(kernel, out_shape, in_specs, flops=1, **kw):
    run = pl.pallas_call(
        kernel,
        out_shape=out_shape,
        in_specs=in_specs,
        cost_estimate=pl.CostEstimate(flops=flops, bytes_accessed=1 << 20, transcendentals=0),
        compiler_params=pltpu.CompilerParams(vmem_limit_bytes=16 << 20),
        **kw,
    )

    def held(*args):
        return run(
            *(
                a if spec is SM else pltpu.with_memory_space_constraint(a, spec.memory_space)
                for a, spec in zip(args, in_specs)
            )
        )

    return held


def copies_kernel(noise, local, out):
    rows = [noise[s, h].astype(F32) for h in range(2) for s in range(8)]
    mine = jnp.concatenate(rows, axis=0).astype(BF16)
    local[...] = mine
    for n in range(out.shape[0]):
        out[n] = mine


def prepare_kernel(bins, ranks, onehot, keep):
    core = lax.axis_index("col_1")
    lane = lax.broadcasted_iota(jnp.int32, (1, 128), 1)
    for i in range(keep.shape[0]):
        slot = 2 * (core * keep.shape[0] + i)
        limit = jnp.where(lane < 64, ranks[0, slot], ranks[0, slot + 1] + 64)
        keep[i] = jnp.where(lane < limit, 1.0, 0.0)
    bin_at = lax.broadcasted_iota(jnp.int32, (NBIN, 128), 0)

    def step(n, carry):
        at = pl.multiple_of(n * 128, 128)
        ids = jnp.broadcast_to(bins[:, pl.ds(at, 128)], (NBIN, 128))
        onehot[:, pl.ds(at, 128)] = jnp.where(ids == bin_at, 1.0, 0.0).astype(BF16)
        return carry

    lax.fori_loop(0, bins.shape[1] // 128, step, 0, unroll=4)


def stage_kernel(source, out, sem):
    copy = pltpu.make_async_copy(source, out, sem)
    copy.start()
    copy.wait()


def spread_kernel(keep, received, noise, other, out):
    blocks = keep.shape[0]
    first = lax.axis_index("col_1") == 0
    own = noise[...].astype(F32)
    far = other[...].astype(F32)
    pieces = (jnp.where(first, own, far).astype(BF16), jnp.where(first, far, own).astype(BF16))
    copies = out.shape[0]
    for i in range(0, blocks, 2):
        total = jnp.concatenate([keep[i] + received[i], keep[i + 1] + received[i + 1]], axis=0)
        top = total.astype(BF16)
        rest = (total - top.astype(F32)).astype(BF16)
        for n in range(copies):
            out[n, 8 * i : 8 * i + 16] = top
            out[n, 8 * (blocks + i) : 8 * (blocks + i) + 16] = rest
    for core in range(2):
        for side in range(2):
            at = 16 * (blocks + 2 * core + side)
            for n in range(copies):
                out[n, at : at + 16] = pieces[core][:, 128 * side : 128 * side + 128]


def project_kernel(columns, right, keep, send):
    row, core = lax.axis_index(ROW), lax.axis_index("col_1")
    tiles = 2 * columns.shape[0]
    groups = right.shape[0] // 8
    lane = lax.broadcasted_iota(jnp.int32, (8, 128), 1)
    for half, out in ((core, keep), (1 - core, send)):
        def step(g, carry, half=half, out=out):
            base = (half * groups + g) * 4
            blocks = []
            low = []
            for n in range(4):
                slot = base + n
                tile = jnp.where(slot < row, slot, slot - row)
                first = tile < tiles // 2
                blocks.append(columns[jnp.where(first, tile, tiles - 1 - tile)])
                low.append(first)
            factor = right[pl.ds(base, 4)].reshape(256, 256)
            full = nt_dot(jnp.concatenate(blocks, axis=0), factor)
            parts = []
            for n in range(4):
                cols = full[16 * n : 16 * n + 16, 128 * (n // 2) : 128 * (n // 2) + 128]
                parts.append(jnp.where(low[n], cols[:8], cols[8:]))
            out[2 * g] = jnp.where(lane < 64, parts[0], parts[1])
            out[2 * g + 1] = jnp.where(lane < 64, parts[2], parts[3])
            return carry

        lax.fori_loop(0, groups, step, 0, unroll=4)


def coeff_kernel(allowed, parts, out):
    blocks = out.shape[0]
    for i in range(0, blocks, 2):
        total = jnp.zeros((16, 128), F32)
        for n in range(parts.shape[0]):
            top = parts[n, 8 * i : 8 * i + 16].astype(F32)
            total = total + (top + parts[n, 8 * (blocks + i) : 8 * (blocks + i) + 16].astype(F32))
        for k in range(2):
            inside = jnp.broadcast_to(allowed[i + k], (8, 128)) > 0.5
            out[i + k] = jnp.where(inside, total[8 * k : 8 * k + 8], 0.0).astype(BF16)


def on_diag_kernel(parts, diag, out):
    col = lax.axis_index(COL)
    span = diag.shape[1]
    pieces = []
    own = jnp.zeros((16, span), F32)
    for n in range(parts.shape[0]):
        for core in range(2):
            at = 256 + 32 * core
            piece = jnp.concatenate([parts[n, at : at + 16], parts[n, at + 16 : at + 32]], axis=1)
            piece = piece.astype(F32)
            number = 2 * n + core
            own = jnp.where(col == number, piece, own)
            pieces.append(jnp.where(number < col, piece, 0.0).astype(BF16))
    before = jnp.concatenate(pieces, axis=1)
    i_at = lax.broadcasted_iota(jnp.int32, (span, span), 0)
    j_at = lax.broadcasted_iota(jnp.int32, (span, span), 1)
    at = pl.multiple_of(col * span, span)
    for h in range(2):
        corner = jnp.where(j_at < i_at, diag[h, :, pl.ds(at, span)].astype(F32), 0.0).astype(BF16)
        total = nt_dot(before, diag[h]) + nt_dot(own.astype(BF16), corner) + own
        out[8 * h : 8 * h + 8] = total[8 * h : 8 * h + 8]


def sample_kernel(mine, theirs, left, on_diag, out):
    row, core = lax.axis_index(ROW), lax.axis_index("col_1")
    blocks = mine.shape[0]
    last = 4 * blocks - 1
    lane = lax.broadcasted_iota(jnp.int32, (8, 128), 1)
    side = jnp.where(lane < 64, 0, 1)
    acc = on_diag[...]
    for half, coeffs in ((core, mine), (1 - core, theirs)):
        rows = []
        for i in range(blocks):
            slot = 2 * (half * blocks + i) + side
            c = coeffs[i].astype(F32)
            upper = jnp.where(slot < row, c, 0.0)
            lower = jnp.where((slot >= row) & (slot < last), c, 0.0)
            rows.append(jnp.concatenate([upper, lower], axis=0).astype(BF16))
        weights = jnp.concatenate(rows, axis=1)
        factor = left[pl.ds(half * blocks, blocks)].reshape(blocks * 128, left.shape[2])
        acc = acc + jnp.dot(weights, factor, preferred_element_type=F32)
    for n in range(out.shape[0]):
        out[n] = acc


def lookup(table, idx):
    low = idx & 127
    bit = [((idx >> (7 + n)) & 1) == 1 for n in range(5)]

    def tree(level, number):
        if level < 0:
            h, piece, half = number >> 4, (number >> 1) & 7, number & 1
            source = table[piece, 8 * h : 8 * h + 8, 128 * half : 128 * half + 128]
            return jnp.take_along_axis(source, low, axis=1, mode="promise_in_bounds")
        zero = tree(level - 1, number)
        one = tree(level - 1, number | (1 << level))
        return jnp.where(bit[level], one, zero)

    return tree(4, 0)


def own_kernel(table, first, partner, out):
    def step(n, carry):
        at = pl.multiple_of(n * 128, 128)
        a = jnp.broadcast_to(first[:, pl.ds(at, 128)], (8, 128))
        b = jnp.broadcast_to(partner[:, pl.ds(at, 128)], (8, 128))
        other = jnp.where(b >= 4096, lookup(table, b), 0.0)
        out[:, pl.ds(at, 128)] = lookup(table, a) - other
        return carry

    lax.fori_loop(0, first.shape[1] // 128, step, 0, unroll=4)


def put_rows(out, rows):
    for n in range(out.shape[0]):
        for i in range(9):
            out[n, :, 128 * i : 128 * i + 128] = rows[i]


def bin_kernel(prev, partner, base, onehot, out, table, pieces):
    table[...] = prev[...].astype(F32)

    def step(n, carry):
        at = pl.multiple_of(n * 128, 128)
        b = jnp.broadcast_to(partner[:, pl.ds(at, 128)], (8, 128))
        differ = base[:, pl.ds(at, 128)] - jnp.where(b < 4096, lookup(table, b), 0.0)
        value = 0.5 * differ * differ
        top = value.astype(BF16).astype(F32)
        rest = value - top
        mid = rest.astype(BF16).astype(F32)
        stack = jnp.concatenate([top, mid, rest - mid, jnp.ones_like(value)], axis=0)
        pieces[:, pl.ds(at, 128)] = stack.astype(BF16)
        return carry

    lax.fori_loop(0, partner.shape[1] // 128, step, 0, unroll=4)
    total = nt_dot(pieces[...], onehot[...])
    sums = (total[:8] + total[8:16]) + total[16:24]
    put_rows(out, [sums[i : i + 1] for i in range(8)] + [total[24:25]])


def added(parts):
    total = parts[0]
    for n in range(1, parts.shape[0]):
        total = total + parts[n]
    return [total[:, 128 * i : 128 * i + 128] for i in range(9)]


def merge_kernel(parts, out):
    put_rows(out, added(parts))


def finish_kernel(parts, out):
    rows = added(parts)
    out[...] = jnp.concatenate(rows[:8], axis=0) / jnp.maximum(rows[8], 1.0)


def vmem(shape, dtype):
    return pltpu.VMEM(shape, dtype)


def body(
    noise, diag_factor, left_factor, right_factor, tile_ranks, pair_first, pair_partner, bin_ids
):
    rows = lax.axis_size(ROW)
    cols = lax.axis_size(COL)
    span = noise.shape[3]
    swap = [(0, 1), (1, 0)]
    first, partner, bins = pair_first[0], pair_partner[0], bin_ids[0]
    pairs = first.shape[1]

    local, spread_noise = call(
        copies_kernel,
        (vmem((16, span), BF16), vmem((rows, 16, span), BF16)),
        [VM],
        name="copies",
    )(noise)
    columns = exchange(spread_noise, ROW)
    onehot, allowed = call(
        prepare_kernel,
        (vmem((NBIN, pairs), BF16), vmem((16, 1, 128), F32)),
        [VM, SM],
        flops=1 << 20,
        name="prepare",
    )(bins, tile_ranks)
    other_noise = lax.ppermute(local, "col_1", swap)
    right = call(
        stage_kernel,
        vmem(right_factor.shape[1:], BF16),
        [HB],
        scratch_shapes=[pltpu.SemaphoreType.DMA(())],
        name="stage",
    )(right_factor[0])

    keep, send = call(
        project_kernel,
        (vmem((16, 8, 128), F32), vmem((16, 8, 128), F32)),
        [VM, VM],
        flops=1 << 28,
        name="project",
    )(columns, right)
    received = lax.ppermute(send, "col_1", swap)
    spread = call(
        spread_kernel, vmem((4, 320, 128), BF16), [VM, VM, VM, VM], name="spread"
    )(keep, received, local, other_noise)
    sums = exchange(spread, "col_0")
    mine = call(coeff_kernel, vmem((16, 8, 128), BF16), [VM, VM], name="coeffs")(
        allowed, sums
    )
    theirs = lax.ppermute(mine, "col_1", swap)
    on_diag = call(
        on_diag_kernel, vmem((16, span), F32), [VM, VM], flops=1 << 28, name="ondiag"
    )(sums, diag_factor[:, 0])
    copies = call(
        sample_kernel,
        vmem((cols, 16, span), F32),
        [VM, VM, VM, VM],
        flops=1 << 26,
        name="samples",
    )(mine, theirs, left_factor[0].reshape(32, 128, span), on_diag)
    samples = jnp.transpose(copies[0].reshape(2, 8, span), (1, 0, 2))[:, :, None]

    own_tiles = exchange(copies, COL)
    prev_tiles = lax.ppermute(
        own_tiles.astype(BF16), ROW, [(source, source + 1) for source in range(rows - 1)]
    )
    base = call(own_kernel, vmem((8, pairs), F32), [VM, VM, VM], flops=1 << 26, name="own")(
        own_tiles, first, partner
    )
    partial = call(
        bin_kernel,
        vmem((lax.axis_size(ZC), 1, 9 * NBIN), F32),
        [VM, VM, VM, VM],
        flops=1 << 26,
        scratch_shapes=[
            pltpu.VMEM((cols, 16, span), F32),
            pltpu.VMEM((32, pairs), BF16),
        ],
        name="bins",
    )(prev_tiles, partner, base, onehot)
    merged = call(merge_kernel, vmem((lax.axis_size(XY), 1, 9 * NBIN), F32), [VM], name="merge")(
        exchange(partial, ZC)
    )
    variogram = call(finish_kernel, jax.ShapeDtypeStruct((8, NBIN), F32), [VM], name="finish")(exchange(merged, XY))
    return (samples, variogram)


def solution(mesh):
    split = Mesh(mesh.devices.reshape(4, 2, 4, 4, 2), ("row_0", "row_1", "row_2", "col_0", "col_1"))
    return jax.shard_map(
        body,
        mesh=split,
        in_specs=(
            P(None, None, ROW, COL),
            P(None, ROW, COL, None),
            P(ROW, None, None, COL),
            P(ROW, None, None, COL),
            P(ROW, None),
            P(ROW, COL, None),
            P(ROW, COL, None),
            P(ROW, COL, None),
        ),
        out_specs=(P(None, None, ROW, COL), P()),
        check_vma=False,
    )
```

```python
import functools

import jax
import jax.numpy as jnp
from jax import lax
from jax.experimental import pallas as pl
from jax.experimental.pallas import tpu as pltpu
from jax.sharding import Mesh
from jax.sharding import PartitionSpec as P

NBIN = 128
ROW = ("row_0", "row_1", "row_2")
COL = ("col_0", "col_1")
XY = ("row_0", "row_2")
ZC = ("row_1", "col_0", "col_1")
F32 = jnp.float32
BF16 = jnp.bfloat16


def exchange(copies, axis):
    return lax.all_to_all(copies, axis, 0, 0, tiled=True)


def nt_dot(a, b):
    return lax.dot_general(a, b, (((1,), (1,)), ((), ())), preferred_element_type=F32)


HB = pl.BlockSpec(memory_space=pltpu.HBM)
VM = pl.BlockSpec(memory_space=pltpu.VMEM)
SM = pl.BlockSpec(memory_space=pltpu.SMEM)


def call(kernel, out_shape, in_specs, flops=1, **kw):
    run = pl.pallas_call(
        kernel,
        out_shape=out_shape,
        in_specs=in_specs,
        cost_estimate=pl.CostEstimate(flops=flops, bytes_accessed=1 << 20, transcendentals=0),
        compiler_params=pltpu.CompilerParams(vmem_limit_bytes=16 << 20),
        **kw,
    )

    def held(*args):
        return run(
            *(
                a if spec is SM else pltpu.with_memory_space_constraint(a, spec.memory_space)
                for a, spec in zip(args, in_specs)
            )
        )

    return held


def copies_kernel(noise, local, out):
    rows = [noise[s, h].astype(F32) for h in range(2) for s in range(8)]
    mine = jnp.concatenate(rows, axis=0).astype(BF16)
    local[...] = mine
    for n in range(out.shape[0]):
        out[n] = mine


def prepare_kernel(bins, ranks, onehot, keep):
    core = lax.axis_index("col_1")
    lane = lax.broadcasted_iota(jnp.int32, (1, 128), 1)
    for i in range(keep.shape[0]):
        slot = 2 * (core * keep.shape[0] + i)
        limit = jnp.where(lane < 64, ranks[0, slot], ranks[0, slot + 1] + 64)
        keep[i] = jnp.where(lane < limit, 1.0, 0.0)
    bin_at = lax.broadcasted_iota(jnp.int32, (NBIN, 128), 0)

    def step(n, carry):
        at = pl.multiple_of(n * 128, 128)
        ids = jnp.broadcast_to(bins[:, pl.ds(at, 128)], (NBIN, 128))
        onehot[:, pl.ds(at, 128)] = jnp.where(ids == bin_at, 1.0, 0.0).astype(BF16)
        return carry

    lax.fori_loop(0, bins.shape[1] // 128, step, 0, unroll=4)


def stage_kernel(source, out, sem):
    copy = pltpu.make_async_copy(source, out, sem)
    copy.start()
    copy.wait()


def spread_kernel(keep, received, noise, other, out):
    blocks = keep.shape[0]
    first = lax.axis_index("col_1") == 0
    own = noise[...].astype(F32)
    far = other[...].astype(F32)
    pieces = (jnp.where(first, own, far).astype(BF16), jnp.where(first, far, own).astype(BF16))
    copies = out.shape[0]
    for i in range(0, blocks, 2):
        total = jnp.concatenate([keep[i] + received[i], keep[i + 1] + received[i + 1]], axis=0)
        top = total.astype(BF16)
        rest = (total - top.astype(F32)).astype(BF16)
        for n in range(copies):
            out[n, 8 * i : 8 * i + 16] = top
            out[n, 8 * (blocks + i) : 8 * (blocks + i) + 16] = rest
    for core in range(2):
        for side in range(2):
            at = 16 * (blocks + 2 * core + side)
            for n in range(copies):
                out[n, at : at + 16] = pieces[core][:, 128 * side : 128 * side + 128]


def project_kernel(columns, right, out, *, away):
    row, core = lax.axis_index(ROW), lax.axis_index("col_1")
    half = 1 - core if away else core
    tiles = 2 * columns.shape[0]
    groups = right.shape[0] // 8
    lane = lax.broadcasted_iota(jnp.int32, (8, 128), 1)

    def step(g, carry):
        base = (half * groups + g) * 4
        blocks = []
        low = []
        for n in range(4):
            slot = base + n
            tile = jnp.where(slot < row, slot, slot - row)
            first = tile < tiles // 2
            blocks.append(columns[jnp.where(first, tile, tiles - 1 - tile)])
            low.append(first)
        factor = right[pl.ds(base, 4)].reshape(256, 256)
        full = nt_dot(jnp.concatenate(blocks, axis=0), factor)
        parts = []
        for n in range(4):
            cols = full[16 * n : 16 * n + 16, 128 * (n // 2) : 128 * (n // 2) + 128]
            parts.append(jnp.where(low[n], cols[:8], cols[8:]))
        out[2 * g] = jnp.where(lane < 64, parts[0], parts[1])
        out[2 * g + 1] = jnp.where(lane < 64, parts[2], parts[3])
        return carry

    lax.fori_loop(0, groups, step, 0, unroll=4)


def coeff_kernel(allowed, parts, out):
    blocks = out.shape[0]
    for i in range(0, blocks, 2):
        total = jnp.zeros((16, 128), F32)
        for n in range(parts.shape[0]):
            top = parts[n, 8 * i : 8 * i + 16].astype(F32)
            total = total + (top + parts[n, 8 * (blocks + i) : 8 * (blocks + i) + 16].astype(F32))
        for k in range(2):
            inside = jnp.broadcast_to(allowed[i + k], (8, 128)) > 0.5
            out[i + k] = jnp.where(inside, total[8 * k : 8 * k + 8], 0.0).astype(BF16)


def on_diag_kernel(parts, diag, out):
    col = lax.axis_index(COL)
    span = diag.shape[1]
    pieces = []
    own = jnp.zeros((16, span), F32)
    for n in range(parts.shape[0]):
        for core in range(2):
            at = 256 + 32 * core
            piece = jnp.concatenate([parts[n, at : at + 16], parts[n, at + 16 : at + 32]], axis=1)
            piece = piece.astype(F32)
            number = 2 * n + core
            own = jnp.where(col == number, piece, own)
            pieces.append(jnp.where(number < col, piece, 0.0).astype(BF16))
    before = jnp.concatenate(pieces, axis=1)
    i_at = lax.broadcasted_iota(jnp.int32, (span, span), 0)
    j_at = lax.broadcasted_iota(jnp.int32, (span, span), 1)
    at = pl.multiple_of(col * span, span)
    for h in range(2):
        corner = jnp.where(j_at < i_at, diag[h, :, pl.ds(at, span)].astype(F32), 0.0).astype(BF16)
        total = nt_dot(before, diag[h]) + nt_dot(own.astype(BF16), corner) + own
        out[8 * h : 8 * h + 8] = total[8 * h : 8 * h + 8]


def sample_kernel(mine, theirs, left, on_diag, out, samples):
    row, core = lax.axis_index(ROW), lax.axis_index("col_1")
    blocks = mine.shape[0]
    last = 4 * blocks - 1
    lane = lax.broadcasted_iota(jnp.int32, (8, 128), 1)
    side = jnp.where(lane < 64, 0, 1)
    acc = on_diag[...]
    for half, coeffs in ((core, mine), (1 - core, theirs)):
        rows = []
        for i in range(blocks):
            slot = 2 * (half * blocks + i) + side
            c = coeffs[i].astype(F32)
            upper = jnp.where(slot < row, c, 0.0)
            lower = jnp.where((slot >= row) & (slot < last), c, 0.0)
            rows.append(jnp.concatenate([upper, lower], axis=0).astype(BF16))
        weights = jnp.concatenate(rows, axis=1)
        factor = left[pl.ds(half * blocks, blocks)].reshape(blocks * 128, left.shape[2])
        acc = acc + jnp.dot(weights, factor, preferred_element_type=F32)
    samples[...] = acc
    for n in range(out.shape[0]):
        out[n] = acc.astype(BF16)


def pack(table, words):
    tiles = [
        [table[p, 8 * h : 8 * h + 8].astype(F32) for h in range(2)] for p in range(table.shape[0])
    ]
    top = jnp.abs(tiles[0][0])
    for pair in tiles:
        for tile in pair:
            top = jnp.maximum(top, jnp.abs(tile))
    top = jnp.maximum(jnp.max(top, axis=1, keepdims=True), 1e-30)
    scale = 32700.0 / top
    for p, pair in enumerate(tiles):
        upper, lower = (jnp.round(tile * scale).astype(jnp.int32) for tile in pair)
        words[p] = (upper << 16) | (lower & 0xFFFF)
    return jnp.broadcast_to(top * (1.0 / 32700.0), (8, 128))


def lookup(words, unit, idx):
    low = idx & 127
    bit = [((idx >> (7 + n)) & 1) == 1 for n in range(5)]

    def tree(level, number):
        if level < 0:
            piece, half = number >> 1, number & 1
            source = words[piece, :, 128 * half : 128 * half + 128]
            return jnp.take_along_axis(source, low, axis=1, mode="promise_in_bounds")
        return jnp.where(bit[level], tree(level - 1, number | (1 << level)), tree(level - 1, number))

    word = tree(3, 0)
    return (jnp.where(bit[4], word << 16, word) >> 16).astype(F32) * unit


def own_kernel(table, first, partner, out, words):
    unit = pack(table, words)

    def step(n, carry):
        at = pl.multiple_of(n * 128, 128)
        a = jnp.broadcast_to(first[:, pl.ds(at, 128)], (8, 128))
        b = jnp.broadcast_to(partner[:, pl.ds(at, 128)], (8, 128))
        other = jnp.where(b >= 4096, lookup(words, unit, b), 0.0)
        out[:, pl.ds(at, 128)] = lookup(words, unit, a) - other
        return carry

    lax.fori_loop(0, first.shape[1] // 128, step, 0, unroll=8)


def emit_kernel(samples, out):
    for h in range(2):
        for s in range(8):
            out[s, h] = samples[8 * h + s : 8 * h + s + 1]


def put_rows(out, rows):
    for n in range(out.shape[0]):
        for i in range(9):
            out[n, :, 128 * i : 128 * i + 128] = rows[i]


def bin_kernel(prev, partner, base, onehot, out, words, pieces):
    unit = pack(prev, words)

    def step(n, carry):
        at = pl.multiple_of(n * 128, 128)
        b = jnp.broadcast_to(partner[:, pl.ds(at, 128)], (8, 128))
        differ = base[:, pl.ds(at, 128)] - jnp.where(b < 4096, lookup(words, unit, b), 0.0)
        value = 0.5 * differ * differ
        top = value.astype(BF16).astype(F32)
        rest = value - top
        mid = rest.astype(BF16).astype(F32)
        stack = jnp.concatenate([top, mid, rest - mid, jnp.ones_like(value)], axis=0)
        pieces[:, pl.ds(at, 128)] = stack.astype(BF16)
        return carry

    lax.fori_loop(0, partner.shape[1] // 128, step, 0, unroll=8)
    total = nt_dot(pieces[...], onehot[...])
    sums = (total[:8] + total[8:16]) + total[16:24]
    put_rows(out, [sums[i : i + 1] for i in range(8)] + [total[24:25]])


def added(parts):
    total = parts[0]
    for n in range(1, parts.shape[0]):
        total = total + parts[n]
    return [total[:, 128 * i : 128 * i + 128] for i in range(9)]


def merge_kernel(parts, out):
    put_rows(out, added(parts))


def finish_kernel(parts, out):
    rows = added(parts)
    out[...] = jnp.concatenate(rows[:8], axis=0) / jnp.maximum(rows[8], 1.0)


def vmem(shape, dtype):
    return pltpu.VMEM(shape, dtype)


def body(
    noise, diag_factor, left_factor, right_factor, tile_ranks, pair_first, pair_partner, bin_ids
):
    rows = lax.axis_size(ROW)
    cols = lax.axis_size(COL)
    span = noise.shape[3]
    swap = [(0, 1), (1, 0)]
    first, partner, bins = pair_first[0], pair_partner[0], bin_ids[0]
    pairs = first.shape[1]

    local, spread_noise = call(
        copies_kernel,
        (vmem((16, span), BF16), vmem((rows, 16, span), BF16)),
        [VM],
        name="copies",
    )(noise)
    columns = exchange(spread_noise, ROW)
    onehot, allowed = call(
        prepare_kernel,
        (vmem((NBIN, pairs), BF16), vmem((16, 1, 128), F32)),
        [VM, SM],
        flops=1 << 20,
        name="prepare",
    )(bins, tile_ranks)
    other_noise = lax.ppermute(local, "col_1", swap)
    right = call(
        stage_kernel,
        vmem(right_factor.shape[1:], BF16),
        [HB],
        scratch_shapes=[pltpu.SemaphoreType.DMA(())],
        name="stage",
    )(right_factor[0])

    def project(away, name):
        return call(
            functools.partial(project_kernel, away=away),
            vmem((16, 8, 128), F32),
            [VM, VM],
            flops=1 << 28,
            name=name,
        )(columns, right)

    send = project(True, "send")
    received = lax.ppermute(send, "col_1", swap)
    keep = project(False, "keep")
    spread = call(
        spread_kernel, vmem((4, 320, 128), BF16), [VM, VM, VM, VM], name="spread"
    )(keep, received, local, other_noise)
    sums = exchange(spread, "col_0")
    mine = call(coeff_kernel, vmem((16, 8, 128), BF16), [VM, VM], name="coeffs")(
        allowed, sums
    )
    theirs = lax.ppermute(mine, "col_1", swap)
    on_diag = call(
        on_diag_kernel, vmem((16, span), F32), [VM, VM], flops=1 << 28, name="ondiag"
    )(sums, diag_factor[:, 0])
    copies, own_samples = call(
        sample_kernel,
        (vmem((cols, 16, span), BF16), vmem((16, span), F32)),
        [VM, VM, VM, VM],
        flops=1 << 26,
        name="samples",
    )(mine, theirs, left_factor[0].reshape(32, 128, span), on_diag)
    own_tiles = exchange(copies, COL)
    prev_tiles = lax.ppermute(own_tiles, ROW, [(source, source + 1) for source in range(rows - 1)])
    samples = call(
        emit_kernel, jax.ShapeDtypeStruct((8, 2, 1, span), F32), [VM], name="emit"
    )(own_samples)
    base = call(
        own_kernel,
        vmem((8, pairs), F32),
        [VM, VM, VM],
        flops=1 << 26,
        scratch_shapes=[pltpu.VMEM((cols, 8, span), jnp.int32)],
        name="own",
    )(own_tiles, first, partner)
    partial = call(
        bin_kernel,
        vmem((lax.axis_size(ZC), 1, 9 * NBIN), F32),
        [VM, VM, VM, VM],
        flops=1 << 26,
        scratch_shapes=[
            pltpu.VMEM((cols, 8, span), jnp.int32),
            pltpu.VMEM((32, pairs), BF16),
        ],
        name="bins",
    )(prev_tiles, partner, base, onehot)
    merged = call(merge_kernel, vmem((lax.axis_size(XY), 1, 9 * NBIN), F32), [VM], name="merge")(
        exchange(partial, ZC)
    )
    variogram = call(finish_kernel, jax.ShapeDtypeStruct((8, NBIN), F32), [VM], name="finish")(exchange(merged, XY))
    return (samples, variogram)


def solution(mesh):
    split = Mesh(mesh.devices.reshape(4, 2, 4, 4, 2), ("row_0", "row_1", "row_2", "col_0", "col_1"))
    return jax.shard_map(
        body,
        mesh=split,
        in_specs=(
            P(None, None, ROW, COL),
            P(None, ROW, COL, None),
            P(ROW, None, None, COL),
            P(ROW, None, None, COL),
            P(ROW, None),
            P(ROW, COL, None),
            P(ROW, COL, None),
            P(ROW, COL, None),
        ),
        out_specs=(P(None, None, ROW, COL), P()),
        check_vma=False,
    )
```

```python
import functools

import jax
import jax.numpy as jnp
from jax import lax
from jax.experimental import pallas as pl
from jax.experimental.pallas import tpu as pltpu
from jax.sharding import Mesh
from jax.sharding import PartitionSpec as P

NBIN = 128
ROW = ("row_0", "row_1", "row_2")
COL = ("col_0", "col_1")
XY = ("row_0", "row_2")
ZC = ("row_1", "col_0", "col_1")
F32 = jnp.float32
F16 = jnp.float16
SUM_UNIT = 128.0
NOISE_UNIT = 1024.0
TURNS = (1, 3, 2)
BF16 = jnp.bfloat16


def exchange(copies, axis):
    return lax.all_to_all(copies, axis, 0, 0, tiled=True)


def nt_dot(a, b):
    return lax.dot_general(a, b, (((1,), (1,)), ((), ())), preferred_element_type=F32)


HB = pl.BlockSpec(memory_space=pltpu.HBM)
VM = pl.BlockSpec(memory_space=pltpu.VMEM)
RAW = pl.BlockSpec(memory_space=pltpu.VMEM)
SM = pl.BlockSpec(memory_space=pltpu.SMEM)


def call(kernel, out_shape, in_specs, flops=1, **kw):
    run = pl.pallas_call(
        kernel,
        out_shape=out_shape,
        in_specs=in_specs,
        cost_estimate=pl.CostEstimate(flops=flops, bytes_accessed=1 << 20, transcendentals=0),
        compiler_params=pltpu.CompilerParams(vmem_limit_bytes=16 << 20),
        **kw,
    )

    def held(*args):
        return run(
            *(
                a if spec is SM or spec is RAW else pltpu.with_memory_space_constraint(a, spec.memory_space)
                for a, spec in zip(args, in_specs)
            )
        )

    return held


def copies_kernel(noise, local, out):
    rows = [noise[s].astype(F32)[h : h + 1] for h in range(2) for s in range(8)]
    mine = jnp.concatenate(rows, axis=0).astype(BF16)
    local[...] = mine
    for n in range(out.shape[0]):
        out[n] = mine


def prepare_kernel(bins, ranks, onehot, keep):
    core = lax.axis_index("col_1")
    lane = lax.broadcasted_iota(jnp.int32, (1, 256), 1)
    for i in range(keep.shape[0]):
        slot = 4 * (core * keep.shape[0] + i)
        limit = ranks[0, slot + 3] + 192
        for n in (2, 1, 0):
            limit = jnp.where(lane < 64 * n + 64, ranks[0, slot + n] + 64 * n, limit)
        keep[i] = jnp.where(lane < limit, 1.0, 0.0)
    bin_at = lax.broadcasted_iota(jnp.int32, (NBIN, 128), 0)

    def step(n, carry):
        at = pl.multiple_of(n * 128, 128)
        ids = jnp.broadcast_to(bins[:, pl.ds(at, 128)], (NBIN, 128))
        onehot[:, pl.ds(at, 128)] = jnp.where(ids == bin_at, 1.0, 0.0).astype(BF16)
        return carry

    lax.fori_loop(0, bins.shape[1] // 128, step, 0, unroll=4)


def stage_kernel(source, out, sem):
    copy = pltpu.make_async_copy(source, out, sem)
    copy.start()
    copy.wait()


def project_kernel(columns, right, out, *, away):
    row, core = lax.axis_index(ROW), lax.axis_index("col_1")
    half = 1 - core if away else core
    tiles = 2 * columns.shape[0]
    groups = right.shape[0] // 8
    lane = lax.broadcasted_iota(jnp.int32, (8, 128), 1)

    def step(g, carry):
        base = (half * groups + g) * 4
        blocks = []
        low = []
        for n in range(4):
            slot = base + n
            tile = jnp.where(slot < row, slot, slot - row)
            first = tile < tiles // 2
            blocks.append(columns[jnp.where(first, tile, tiles - 1 - tile)])
            low.append(first)
        factor = right[pl.ds(base, 4)].reshape(256, 256)
        full = nt_dot(jnp.concatenate(blocks, axis=0), factor)
        parts = []
        for n in range(4):
            cols = full[16 * n : 16 * n + 16, 128 * (n // 2) : 128 * (n // 2) + 128]
            parts.append(jnp.where(low[n], cols[:8], cols[8:]))
        out[g, :, :128] = jnp.where(lane < 64, parts[0], parts[1])
        out[g, :, 128:] = jnp.where(lane < 64, parts[2], parts[3])
        return carry

    lax.fori_loop(0, groups, step, 0, unroll=4)


def on_diag_kernel(n0, n1, n2, n3, diag, out):
    col, chip = lax.axis_index(COL), lax.axis_index("col_0")
    span = diag.shape[1]
    own = jnp.where(lax.axis_index("col_1") == 0, n0[:16].astype(F32), n0[16:].astype(F32))
    i_at = lax.broadcasted_iota(jnp.int32, (span, span), 0)
    j_at = lax.broadcasted_iota(jnp.int32, (span, span), 1)
    acc = [own, own]
    at = pl.multiple_of(col * span, span)
    for h in range(2):
        corner = jnp.where(j_at < i_at, diag[h, :, pl.ds(at, span)].astype(F32), 0.0).astype(BF16)
        acc[h] = acc[h] + nt_dot(own.astype(BF16), corner)
    for noise, turn in zip((n0, n1, n2, n3), (0, *TURNS)):
        for core in range(2):
            number = 2 * lax.rem(chip + 4 - turn, 4) + core
            piece = noise[16 * core : 16 * core + 16].astype(F32)
            piece = jnp.where(number < col, piece, 0.0).astype(BF16)
            from_ = pl.multiple_of(number * span, span)
            for h in range(2):
                acc[h] = acc[h] + nt_dot(piece, diag[h, :, pl.ds(from_, span)])
    for h in range(2):
        out[8 * h : 8 * h + 8] = acc[h][8 * h : 8 * h + 8]


def sample_kernel(mine, theirs, left, on_diag, out, samples):
    row, core = lax.axis_index(ROW), lax.axis_index("col_1")
    blocks = mine.shape[0]
    last = 8 * blocks - 1
    side = lax.broadcasted_iota(jnp.int32, (8, 256), 1) >> 6
    acc = on_diag[...]
    for half, coeffs in ((core, mine), (1 - core, theirs)):
        rows = []
        for i in range(blocks):
            slot = 4 * (half * blocks + i) + side
            c = coeffs[i].astype(F32)
            upper = jnp.where(slot < row, c, 0.0)
            lower = jnp.where((slot >= row) & (slot < last), c, 0.0)
            rows.append(jnp.concatenate([upper, lower], axis=0).astype(BF16))
        weights = jnp.concatenate(rows, axis=1)
        factor = left[pl.ds(half * blocks, blocks)].reshape(blocks * 256, left.shape[2])
        acc = acc + jnp.dot(weights, factor, preferred_element_type=F32)
    samples[...] = acc
    for n in range(out.shape[0]):
        out[n] = acc.astype(BF16)


def pack(table, words):
    tiles = [
        [table[p, 8 * h : 8 * h + 8].astype(F32) for h in range(2)] for p in range(table.shape[0])
    ]
    top = jnp.abs(tiles[0][0])
    for pair in tiles:
        for tile in pair:
            top = jnp.maximum(top, jnp.abs(tile))
    top = jnp.maximum(jnp.max(top, axis=1, keepdims=True), 1e-30)
    scale = 32700.0 / top
    for p, pair in enumerate(tiles):
        upper, lower = (jnp.round(tile * scale).astype(jnp.int32) for tile in pair)
        words[p] = (upper << 16) | (lower & 0xFFFF)
    return jnp.broadcast_to(top * (1.0 / 32700.0), (8, 128))


def lookup(words, unit, idx):
    low = idx & 127
    bit = [((idx >> (7 + n)) & 1) == 1 for n in range(5)]

    def tree(level, number):
        if level < 0:
            piece, half = number >> 1, number & 1
            source = words[piece, :, 128 * half : 128 * half + 128]
            return jnp.take_along_axis(source, low, axis=1, mode="promise_in_bounds")
        return jnp.where(bit[level], tree(level - 1, number | (1 << level)), tree(level - 1, number))

    word = tree(3, 0)
    return (jnp.where(bit[4], word << 16, word) >> 16).astype(F32) * unit


def own_kernel(table, first, partner, out, words):
    unit = pack(table, words)

    def step(n, carry):
        at = pl.multiple_of(n * 128, 128)
        a = jnp.broadcast_to(first[:, pl.ds(at, 128)], (8, 128))
        b = jnp.broadcast_to(partner[:, pl.ds(at, 128)], (8, 128))
        other = jnp.where(b >= 4096, lookup(words, unit, b), 0.0)
        out[:, pl.ds(at, 128)] = lookup(words, unit, a) - other
        return carry

    lax.fori_loop(0, first.shape[1] // 128, step, 0, unroll=8)


def emit_kernel(samples, out):
    for h in range(2):
        for s in range(8):
            out[s, h] = samples[8 * h + s : 8 * h + s + 1]


def put_rows(out, rows):
    for n in range(out.shape[0]):
        for i in range(9):
            out[n, :, 128 * i : 128 * i + 128] = rows[i]


def bin_kernel(prev, partner, base, onehot, out, words, pieces):
    unit = pack(prev, words)

    def step(n, carry):
        at = pl.multiple_of(n * 128, 128)
        b = jnp.broadcast_to(partner[:, pl.ds(at, 128)], (8, 128))
        differ = base[:, pl.ds(at, 128)] - jnp.where(b < 4096, lookup(words, unit, b), 0.0)
        value = 0.5 * differ * differ
        top = value.astype(BF16).astype(F32)
        rest = value - top
        mid = rest.astype(BF16).astype(F32)
        stack = jnp.concatenate([top, mid, rest - mid, jnp.ones_like(value)], axis=0)
        pieces[:, pl.ds(at, 128)] = stack.astype(BF16)
        return carry

    lax.fori_loop(0, partner.shape[1] // 128, step, 0, unroll=8)
    total = nt_dot(pieces[...], onehot[...])
    sums = (total[:8] + total[8:16]) + total[16:24]
    put_rows(out, [sums[i : i + 1] for i in range(8)] + [total[24:25]])


def added(parts):
    total = parts[0]
    for n in range(1, parts.shape[0]):
        total = total + parts[n]
    return [total[:, 128 * i : 128 * i + 128] for i in range(9)]


def merge_kernel(parts, out):
    put_rows(out, added(parts))


def finish_kernel(parts, out):
    rows = added(parts)
    out[...] = jnp.concatenate(rows[:8], axis=0) / jnp.maximum(rows[8], 1.0)


def vmem(shape, dtype):
    return pltpu.VMEM(shape, dtype)


def body(
    noise, diag_factor, left_factor, right_factor, tile_ranks, pair_first, pair_partner, bin_ids
):
    rows = lax.axis_size(ROW)
    cols = lax.axis_size(COL)
    span = noise.shape[3]
    swap = [(0, 1), (1, 0)]
    first, partner, bins = pair_first[0], pair_partner[0], bin_ids[0]
    pairs = first.shape[1]

    local, spread_noise = call(
        copies_kernel,
        (vmem((16, span), BF16), vmem((rows, 16, span), BF16)),
        [RAW],
        name="copies",
    )(jnp.transpose(noise, (0, 2, 1, 3))[:, 0])
    columns = exchange(spread_noise, ROW)
    onehot, allowed = call(
        prepare_kernel,
        (vmem((NBIN, pairs), BF16), vmem((8, 1, 256), F32)),
        [VM, SM],
        flops=1 << 20,
        name="prepare",
    )(bins, tile_ranks)
    other_noise = lax.ppermute(local, "col_1", swap)
    right = call(
        stage_kernel,
        vmem(right_factor.shape[1:], BF16),
        [HB],
        scratch_shapes=[pltpu.SemaphoreType.DMA(())],
        name="stage",
    )(right_factor[0])

    def project(away, name):
        return call(
            functools.partial(project_kernel, away=away),
            vmem((8, 8, 256), F32),
            [VM, VM],
            flops=1 << 28,
            name=name,
        )(columns, right)

    send = project(True, "send")
    received = lax.ppermute(send, "col_1", swap)
    keep = project(False, "keep")
    pair = keep + received
    low_first = lax.axis_index("col_1") == 0
    noises = jnp.where(
        low_first,
        jnp.concatenate([local, other_noise]),
        jnp.concatenate([other_noise, local]),
    )
    noises16 = (noises.astype(F32) * NOISE_UNIT).astype(F16)
    payload = jnp.concatenate([(pair * SUM_UNIT).astype(F16).reshape(64, 256), noises16])
    arrived = []
    for turn in TURNS:
        arrived.append(
            lax.ppermute(payload, "col_0", [(chip, (chip + turn) % 4) for chip in range(4)])
        )
    total = sum(x[:64].astype(F32) for x in arrived).reshape(8, 8, 256) * (1.0 / SUM_UNIT) + pair
    mine = jnp.where(allowed > 0.5, total, 0.0).astype(BF16)
    all_noise = [noises] + [(x[64:].astype(F32) * (1.0 / NOISE_UNIT)).astype(BF16) for x in arrived]
    theirs = lax.ppermute(mine, "col_1", swap)
    on_diag = call(
        on_diag_kernel, vmem((16, span), F32), [VM] * 5, flops=1 << 28, name="ondiag"
    )(*all_noise, diag_factor[:, 0])
    copies, own_samples = call(
        sample_kernel,
        (vmem((cols, 16, span), BF16), vmem((16, span), F32)),
        [VM, VM, VM, VM],
        flops=1 << 26,
        name="samples",
    )(mine, theirs, left_factor[0].reshape(16, 256, span), on_diag)
    own_tiles = exchange(copies, COL)
    prev_tiles = lax.ppermute(own_tiles, ROW, [(source, source + 1) for source in range(rows - 1)])
    samples = call(
        emit_kernel, jax.ShapeDtypeStruct((8, 2, 1, span), F32), [VM], name="emit"
    )(own_samples)
    base = call(
        own_kernel,
        vmem((8, pairs), F32),
        [VM, VM, VM],
        flops=1 << 26,
        scratch_shapes=[pltpu.VMEM((cols, 8, span), jnp.int32)],
        name="own",
    )(own_tiles, first, partner)
    partial = call(
        bin_kernel,
        vmem((lax.axis_size(ZC), 1, 9 * NBIN), F32),
        [VM, VM, VM, VM],
        flops=1 << 26,
        scratch_shapes=[
            pltpu.VMEM((cols, 8, span), jnp.int32),
            pltpu.VMEM((32, pairs), BF16),
        ],
        name="bins",
    )(prev_tiles, partner, base, onehot)
    merged = call(merge_kernel, vmem((lax.axis_size(XY), 1, 9 * NBIN), F32), [VM], name="merge")(
        exchange(partial, ZC)
    )
    variogram = call(finish_kernel, jax.ShapeDtypeStruct((8, NBIN), F32), [VM], name="finish")(exchange(merged, XY))
    return (samples, variogram)


def solution(mesh):
    split = Mesh(mesh.devices.reshape(4, 2, 4, 4, 2), ("row_0", "row_1", "row_2", "col_0", "col_1"))
    return jax.shard_map(
        body,
        mesh=split,
        in_specs=(
            P(None, None, ROW, COL),
            P(None, ROW, COL, None),
            P(ROW, None, None, COL),
            P(ROW, None, None, COL),
            P(ROW, None),
            P(ROW, COL, None),
            P(ROW, COL, None),
            P(ROW, COL, None),
        ),
        out_specs=(P(None, None, ROW, COL), P()),
        check_vma=False,
    )
```

```python
import functools

import jax
import jax.numpy as jnp
from jax import lax
from jax.experimental import pallas as pl
from jax.experimental.pallas import tpu as pltpu
from jax.sharding import Mesh
from jax.sharding import PartitionSpec as P

NBIN = 128
ROW = ("row_0", "row_1", "row_2")
COL = ("col_0", "col_1")
XY = ("row_0", "row_2")
ZC = ("row_1", "col_0", "col_1")
F32 = jnp.float32
F16 = jnp.float16
SUM_UNIT = 128.0
NOISE_UNIT = 1024.0
TURNS = (2, 1, 3)
BF16 = jnp.bfloat16


def exchange(copies, axis):
    return lax.all_to_all(copies, axis, 0, 0, tiled=True)


def nt_dot(a, b):
    return lax.dot_general(a, b, (((1,), (1,)), ((), ())), preferred_element_type=F32)


HB = pl.BlockSpec(memory_space=pltpu.HBM)
VM = pl.BlockSpec(memory_space=pltpu.VMEM)
SM = pl.BlockSpec(memory_space=pltpu.SMEM)


def call(kernel, out_shape, in_specs, flops=1, **kw):
    run = pl.pallas_call(
        kernel,
        out_shape=out_shape,
        in_specs=in_specs,
        cost_estimate=pl.CostEstimate(flops=flops, bytes_accessed=1 << 20, transcendentals=0),
        compiler_params=pltpu.CompilerParams(vmem_limit_bytes=16 << 20),
        **kw,
    )

    def held(*args):
        return run(
            *(
                a if spec is SM else pltpu.with_memory_space_constraint(a, spec.memory_space)
                for a, spec in zip(args, in_specs)
            )
        )

    return held


def copies_kernel(source, local, out, noise, sem):
    copy = pltpu.make_async_copy(source, noise, sem)
    copy.start()
    copy.wait()
    rows = [noise[s].astype(F32)[h : h + 1] for h in range(2) for s in range(8)]
    mine = jnp.concatenate(rows, axis=0).astype(BF16)
    local[...] = mine
    for n in range(out.shape[0]):
        out[n] = mine


def prepare_kernel(bins, ranks, onehot, keep):
    core = lax.axis_index("col_1")
    lane = lax.broadcasted_iota(jnp.int32, (1, 256), 1)
    for i in range(keep.shape[0]):
        slot = 4 * (core * keep.shape[0] + i)
        limit = ranks[0, slot + 3] + 192
        for n in (2, 1, 0):
            limit = jnp.where(lane < 64 * n + 64, ranks[0, slot + n] + 64 * n, limit)
        keep[i] = jnp.where(lane < limit, 1.0, 0.0)
    bin_at = lax.broadcasted_iota(jnp.int32, (NBIN, 128), 0)

    def step(n, carry):
        at = pl.multiple_of(n * 128, 128)
        ids = jnp.broadcast_to(bins[:, pl.ds(at, 128)], (NBIN, 128))
        onehot[:, pl.ds(at, 128)] = jnp.where(ids == bin_at, 1.0, 0.0).astype(BF16)
        return carry

    lax.fori_loop(0, bins.shape[1] // 128, step, 0, unroll=4)


def stage_kernel(source, out, sem):
    copy = pltpu.make_async_copy(source, out, sem)
    copy.start()
    copy.wait()


def project_kernel(columns, right, out, *, away):
    row, core = lax.axis_index(ROW), lax.axis_index("col_1")
    half = 1 - core if away else core
    tiles = 2 * columns.shape[0]
    groups = right.shape[0] // 8
    lane = lax.broadcasted_iota(jnp.int32, (8, 128), 1)

    def step(g, carry):
        base = (half * groups + g) * 4
        blocks = []
        low = []
        for n in range(4):
            slot = base + n
            tile = jnp.where(slot < row, slot, slot - row)
            first = tile < tiles // 2
            blocks.append(columns[jnp.where(first, tile, tiles - 1 - tile)])
            low.append(first)
        factor = right[pl.ds(base, 4)].reshape(256, 256)
        full = nt_dot(jnp.concatenate(blocks, axis=0), factor)
        parts = []
        for n in range(4):
            cols = full[16 * n : 16 * n + 16, 128 * (n // 2) : 128 * (n // 2) + 128]
            parts.append(jnp.where(low[n], cols[:8], cols[8:]))
        out[g, :, :128] = jnp.where(lane < 64, parts[0], parts[1])
        out[g, :, 128:] = jnp.where(lane < 64, parts[2], parts[3])
        return carry

    lax.fori_loop(0, groups, step, 0, unroll=4)


def on_diag_kernel(n0, n1, n2, n3, diag, out):
    col, chip = lax.axis_index(COL), lax.axis_index("col_0")
    span = diag.shape[1]
    own = jnp.where(lax.axis_index("col_1") == 0, n0[:16].astype(F32), n0[16:].astype(F32))
    i_at = lax.broadcasted_iota(jnp.int32, (span, span), 0)
    j_at = lax.broadcasted_iota(jnp.int32, (span, span), 1)
    acc = [own, own]
    at = pl.multiple_of(col * span, span)
    for h in range(2):
        corner = jnp.where(j_at < i_at, diag[h, :, pl.ds(at, span)].astype(F32), 0.0).astype(BF16)
        acc[h] = acc[h] + nt_dot(own.astype(BF16), corner)
    for noise, turn in zip((n0, n1, n2, n3), (0, *TURNS)):
        for core in range(2):
            number = 2 * lax.rem(chip + 4 - turn, 4) + core
            piece = noise[16 * core : 16 * core + 16].astype(F32)
            piece = jnp.where(number < col, piece, 0.0).astype(BF16)
            from_ = pl.multiple_of(number * span, span)
            for h in range(2):
                acc[h] = acc[h] + nt_dot(piece, diag[h, :, pl.ds(from_, span)])
    for h in range(2):
        out[8 * h : 8 * h + 8] = acc[h][8 * h : 8 * h + 8]


def sample_kernel(mine, theirs, left, on_diag, out, samples):
    row, core = lax.axis_index(ROW), lax.axis_index("col_1")
    blocks = mine.shape[0]
    last = 8 * blocks - 1
    side = lax.broadcasted_iota(jnp.int32, (8, 256), 1) >> 6
    acc = on_diag[...]
    for half, coeffs in ((core, mine), (1 - core, theirs)):
        rows = []
        for i in range(blocks):
            slot = 4 * (half * blocks + i) + side
            c = coeffs[i].astype(F32)
            upper = jnp.where(slot < row, c, 0.0)
            lower = jnp.where((slot >= row) & (slot < last), c, 0.0)
            rows.append(jnp.concatenate([upper, lower], axis=0).astype(BF16))
        weights = jnp.concatenate(rows, axis=1)
        factor = left[pl.ds(half * blocks, blocks)].reshape(blocks * 256, left.shape[2])
        acc = acc + jnp.dot(weights, factor, preferred_element_type=F32)
    samples[...] = acc
    for n in range(out.shape[0]):
        out[n] = acc.astype(BF16)


def pack(table, words):
    tiles = [
        [table[p, 8 * h : 8 * h + 8].astype(F32) for h in range(2)] for p in range(table.shape[0])
    ]
    top = jnp.abs(tiles[0][0])
    for pair in tiles:
        for tile in pair:
            top = jnp.maximum(top, jnp.abs(tile))
    top = jnp.maximum(jnp.max(top, axis=1, keepdims=True), 1e-30)
    scale = 32700.0 / top
    for p, pair in enumerate(tiles):
        upper, lower = (jnp.round(tile * scale).astype(jnp.int32) for tile in pair)
        words[p] = (upper << 16) | (lower & 0xFFFF)
    return jnp.broadcast_to(top * (1.0 / 32700.0), (8, 128))


def lookup(words, unit, idx):
    low = idx & 127
    bit = [((idx >> (7 + n)) & 1) == 1 for n in range(5)]

    def tree(level, number):
        if level < 0:
            piece, half = number >> 1, number & 1
            source = words[piece, :, 128 * half : 128 * half + 128]
            return jnp.take_along_axis(source, low, axis=1, mode="promise_in_bounds")
        return jnp.where(bit[level], tree(level - 1, number | (1 << level)), tree(level - 1, number))

    word = tree(3, 0)
    return (jnp.where(bit[4], word << 16, word) >> 16).astype(F32) * unit


def own_kernel(table, first, partner, out, words):
    unit = pack(table, words)

    def step(n, carry):
        at = pl.multiple_of(n * 128, 128)
        a = jnp.broadcast_to(first[:, pl.ds(at, 128)], (8, 128))
        b = jnp.broadcast_to(partner[:, pl.ds(at, 128)], (8, 128))
        other = jnp.where(b >= 4096, lookup(words, unit, b), 0.0)
        out[:, pl.ds(at, 128)] = lookup(words, unit, a) - other
        return carry

    lax.fori_loop(0, first.shape[1] // 128, step, 0, unroll=8)


def emit_kernel(samples, out):
    for h in range(2):
        for s in range(8):
            out[s, h] = samples[8 * h + s : 8 * h + s + 1]


def put_rows(out, rows):
    for n in range(out.shape[0]):
        for i in range(9):
            out[n, :, 128 * i : 128 * i + 128] = rows[i]


def bin_kernel(prev, partner, base, onehot, out, words, pieces):
    unit = pack(prev, words)

    def step(n, carry):
        at = pl.multiple_of(n * 128, 128)
        b = jnp.broadcast_to(partner[:, pl.ds(at, 128)], (8, 128))
        differ = base[:, pl.ds(at, 128)] - jnp.where(b < 4096, lookup(words, unit, b), 0.0)
        value = 0.5 * differ * differ
        top = value.astype(BF16).astype(F32)
        rest = value - top
        mid = rest.astype(BF16).astype(F32)
        stack = jnp.concatenate([top, mid, rest - mid, jnp.ones_like(value)], axis=0)
        pieces[:, pl.ds(at, 128)] = stack.astype(BF16)
        return carry

    lax.fori_loop(0, partner.shape[1] // 128, step, 0, unroll=8)
    total = nt_dot(pieces[...], onehot[...])
    sums = (total[:8] + total[8:16]) + total[16:24]
    put_rows(out, [sums[i : i + 1] for i in range(8)] + [total[24:25]])


def added(parts):
    total = parts[0]
    for n in range(1, parts.shape[0]):
        total = total + parts[n]
    return [total[:, 128 * i : 128 * i + 128] for i in range(9)]


def merge_kernel(parts, out):
    put_rows(out, added(parts))


def finish_kernel(parts, out):
    rows = added(parts)
    out[...] = jnp.concatenate(rows[:8], axis=0) / jnp.maximum(rows[8], 1.0)


def vmem(shape, dtype):
    return pltpu.VMEM(shape, dtype)


def body(
    noise, diag_factor, left_factor, right_factor, tile_ranks, pair_first, pair_partner, bin_ids
):
    rows = lax.axis_size(ROW)
    cols = lax.axis_size(COL)
    span = noise.shape[3]
    swap = [(0, 1), (1, 0)]
    first, partner, bins = pair_first[0], pair_partner[0], bin_ids[0]
    pairs = first.shape[1]

    local, spread_noise = call(
        copies_kernel,
        (vmem((16, span), BF16), vmem((rows, 16, span), BF16)),
        [HB],
        scratch_shapes=[pltpu.VMEM((8, 2, span), BF16), pltpu.SemaphoreType.DMA(())],
        name="copies",
    )(jnp.transpose(noise, (0, 2, 1, 3))[:, 0])
    columns = exchange(spread_noise, ROW)
    onehot, allowed = call(
        prepare_kernel,
        (vmem((NBIN, pairs), BF16), vmem((8, 1, 256), F32)),
        [VM, SM],
        flops=1 << 20,
        name="prepare",
    )(bins, tile_ranks)
    other_noise = lax.ppermute(local, "col_1", swap)
    right = call(
        stage_kernel,
        vmem(right_factor.shape[1:], BF16),
        [HB],
        scratch_shapes=[pltpu.SemaphoreType.DMA(())],
        name="stage",
    )(right_factor[0])

    def project(away, name):
        return call(
            functools.partial(project_kernel, away=away),
            vmem((8, 8, 256), F32),
            [VM, VM],
            flops=1 << 28,
            name=name,
        )(columns, right)

    send = project(True, "send")
    received = lax.ppermute(send, "col_1", swap)
    keep = project(False, "keep")
    pair = keep + received
    low_first = lax.axis_index("col_1") == 0
    noises = jnp.where(
        low_first,
        jnp.concatenate([local, other_noise]),
        jnp.concatenate([other_noise, local]),
    )
    noises16 = (noises.astype(F32) * NOISE_UNIT).astype(F16)
    payload = jnp.concatenate([(pair * SUM_UNIT).astype(F16).reshape(64, 256), noises16])
    arrived = []
    for turn in TURNS:
        arrived.append(
            lax.ppermute(payload, "col_0", [(chip, (chip + turn) % 4) for chip in range(4)])
        )
    total = sum(x[:64].astype(F32) for x in arrived).reshape(8, 8, 256) * (1.0 / SUM_UNIT) + pair
    mine = jnp.where(allowed > 0.5, total, 0.0).astype(BF16)
    all_noise = [noises] + [(x[64:].astype(F32) * (1.0 / NOISE_UNIT)).astype(BF16) for x in arrived]
    theirs = lax.ppermute(mine, "col_1", swap)
    on_diag = call(
        on_diag_kernel, vmem((16, span), F32), [VM] * 5, flops=1 << 28, name="ondiag"
    )(*all_noise, diag_factor[:, 0])
    copies, own_samples = call(
        sample_kernel,
        (vmem((cols, 16, span), BF16), vmem((16, span), F32)),
        [VM, VM, VM, VM],
        flops=1 << 26,
        name="samples",
    )(mine, theirs, left_factor[0].reshape(16, 256, span), on_diag)
    own_tiles = exchange(copies, COL)
    prev_tiles = lax.ppermute(own_tiles, ROW, [(source, source + 1) for source in range(rows - 1)])
    samples = call(
        emit_kernel, jax.ShapeDtypeStruct((8, 2, 1, span), F32), [VM], name="emit"
    )(own_samples)
    base = call(
        own_kernel,
        vmem((8, pairs), F32),
        [VM, VM, VM],
        flops=1 << 26,
        scratch_shapes=[pltpu.VMEM((cols, 8, span), jnp.int32)],
        name="own",
    )(own_tiles, first, partner)
    partial = call(
        bin_kernel,
        vmem((lax.axis_size(ZC), 1, 9 * NBIN), F32),
        [VM, VM, VM, VM],
        flops=1 << 26,
        scratch_shapes=[
            pltpu.VMEM((cols, 8, span), jnp.int32),
            pltpu.VMEM((32, pairs), BF16),
        ],
        name="bins",
    )(prev_tiles, partner, base, onehot)
    merged = call(merge_kernel, vmem((lax.axis_size(XY), 1, 9 * NBIN), F32), [VM], name="merge")(
        exchange(partial, ZC)
    )
    variogram = call(finish_kernel, jax.ShapeDtypeStruct((8, NBIN), F32), [VM], name="finish")(exchange(merged, XY))
    return (samples, variogram)


def solution(mesh):
    split = Mesh(mesh.devices.reshape(4, 2, 4, 4, 2), ("row_0", "row_1", "row_2", "col_0", "col_1"))
    return jax.shard_map(
        body,
        mesh=split,
        in_specs=(
            P(None, None, ROW, COL),
            P(None, ROW, COL, None),
            P(ROW, None, None, COL),
            P(ROW, None, None, COL),
            P(ROW, None),
            P(ROW, COL, None),
            P(ROW, COL, None),
            P(ROW, COL, None),
        ),
        out_specs=(P(None, None, ROW, COL), P()),
        check_vma=False,
    )
```

```python
import functools

import jax
import jax.numpy as jnp
from jax import lax
from jax.experimental import pallas as pl
from jax.experimental.pallas import tpu as pltpu
from jax.sharding import Mesh
from jax.sharding import PartitionSpec as P

NBIN = 128
ROW = ("row_0", "row_1", "row_2")
COL = ("col_0", "col_1")
XY = ("row_0", "row_2")
ZC = ("row_1", "col_0", "col_1")
F32 = jnp.float32
F16 = jnp.float16
SUM_UNIT = 128.0
NOISE_UNIT = 1024.0
TURNS = (2, 1, 3)
BF16 = jnp.bfloat16


def exchange(copies, axis):
    return lax.all_to_all(copies, axis, 0, 0, tiled=True)


def nt_dot(a, b):
    return lax.dot_general(a, b, (((1,), (1,)), ((), ())), preferred_element_type=F32)


HB = pl.BlockSpec(memory_space=pltpu.HBM)
VM = pl.BlockSpec(memory_space=pltpu.VMEM)
SM = pl.BlockSpec(memory_space=pltpu.SMEM)


def call(kernel, out_shape, in_specs, flops=1, **kw):
    run = pl.pallas_call(
        kernel,
        out_shape=out_shape,
        in_specs=in_specs,
        cost_estimate=pl.CostEstimate(flops=flops, bytes_accessed=1 << 20, transcendentals=0),
        compiler_params=pltpu.CompilerParams(vmem_limit_bytes=16 << 20),
        **kw,
    )

    def held(*args):
        return run(
            *(
                a if spec is SM else pltpu.with_memory_space_constraint(a, spec.memory_space)
                for a, spec in zip(args, in_specs)
            )
        )

    return held


def copies_kernel(source, local, out, noise, sem):
    copy = pltpu.make_async_copy(source, noise, sem)
    copy.start()
    copy.wait()
    rows = [noise[s].astype(F32)[h : h + 1] for h in range(2) for s in range(8)]
    mine = jnp.concatenate(rows, axis=0).astype(BF16)
    local[...] = mine
    for n in range(out.shape[0]):
        out[n] = mine


def prepare_kernel(bins, ranks, onehot, keep, counts):
    core = lax.axis_index("col_1")
    lane = lax.broadcasted_iota(jnp.int32, (1, 256), 1)
    for i in range(keep.shape[0]):
        slot = 4 * (core * keep.shape[0] + i)
        limit = ranks[0, slot + 3] + 192
        for n in (2, 1, 0):
            limit = jnp.where(lane < 64 * n + 64, ranks[0, slot + n] + 64 * n, limit)
        keep[i] = jnp.where(lane < limit, 1.0, 0.0)
    bin_at = lax.broadcasted_iota(jnp.int32, (NBIN, 128), 0)

    def step(n, carry):
        at = pl.multiple_of(n * 128, 128)
        ids = jnp.broadcast_to(bins[:, pl.ds(at, 128)], (NBIN, 128))
        onehot[:, pl.ds(at, 128)] = jnp.where(ids == bin_at, 1.0, 0.0).astype(BF16)
        return carry

    lax.fori_loop(0, bins.shape[1] // 128, step, 0, unroll=4)
    counts[...] = nt_dot(jnp.ones((8, onehot.shape[1]), BF16), onehot[...])


def order_kernel(local, other, out):
    first = lax.axis_index("col_1") == 0
    own = local[...].astype(F32)
    far = other[...].astype(F32)
    out[:16] = jnp.where(first, own, far).astype(BF16)
    out[16:] = jnp.where(first, far, own).astype(BF16)


def project_kernel(columns, right, out, factors, sems, *, away):
    row, core = lax.axis_index(ROW), lax.axis_index("col_1")
    half = 1 - core if away else core
    tiles = 2 * columns.shape[0]
    groups = out.shape[0]
    lane = lax.broadcasted_iota(jnp.int32, (8, 128), 1)
    base = half * groups * 4
    loads = [
        pltpu.make_async_copy(right.at[pl.ds(base + 4 * g, 4)], factors.at[g], sems.at[g])
        for g in range(groups)
    ]
    for load in loads:
        load.start()
    for g in range(groups):
        blocks = []
        low = []
        for n in range(4):
            slot = base + 4 * g + n
            tile = jnp.where(slot < row, slot, slot - row)
            first = tile < tiles // 2
            blocks.append(columns[jnp.where(first, tile, tiles - 1 - tile)])
            low.append(first)
        loads[g].wait()
        full = nt_dot(jnp.concatenate(blocks, axis=0), factors[g].reshape(256, 256))
        parts = []
        for n in range(4):
            cols = full[16 * n : 16 * n + 16, 128 * (n // 2) : 128 * (n // 2) + 128]
            parts.append(jnp.where(low[n], cols[:8], cols[8:]))
        out[g, :, :128] = jnp.where(lane < 64, parts[0], parts[1])
        out[g, :, 128:] = jnp.where(lane < 64, parts[2], parts[3])


def on_diag_kernel(n0, n1, n2, n3, diag, out):
    col, chip = lax.axis_index(COL), lax.axis_index("col_0")
    span = diag.shape[1]
    own = jnp.where(lax.axis_index("col_1") == 0, n0[:16].astype(F32), n0[16:].astype(F32))
    i_at = lax.broadcasted_iota(jnp.int32, (span, span), 0)
    j_at = lax.broadcasted_iota(jnp.int32, (span, span), 1)
    acc = [own, own]
    at = pl.multiple_of(col * span, span)
    for h in range(2):
        corner = jnp.where(j_at < i_at, diag[h, :, pl.ds(at, span)].astype(F32), 0.0).astype(BF16)
        acc[h] = acc[h] + nt_dot(own.astype(BF16), corner)
    for noise, turn in zip((n0, n1, n2, n3), (0, *TURNS)):
        for core in range(2):
            number = 2 * lax.rem(chip + 4 - turn, 4) + core
            piece = noise[16 * core : 16 * core + 16].astype(F32)
            piece = jnp.where(number < col, piece, 0.0).astype(BF16)
            from_ = pl.multiple_of(number * span, span)
            for h in range(2):
                acc[h] = acc[h] + nt_dot(piece, diag[h, :, pl.ds(from_, span)])
    for h in range(2):
        out[8 * h : 8 * h + 8] = acc[h][8 * h : 8 * h + 8]


def sample_kernel(mine, theirs, left, on_diag, out, samples):
    row, core = lax.axis_index(ROW), lax.axis_index("col_1")
    blocks = mine.shape[0]
    last = 8 * blocks - 1
    side = lax.broadcasted_iota(jnp.int32, (8, 256), 1) >> 6
    acc = on_diag[...]
    for half, coeffs in ((core, mine), (1 - core, theirs)):
        rows = []
        for i in range(blocks):
            slot = 4 * (half * blocks + i) + side
            c = coeffs[i].astype(F32)
            upper = jnp.where(slot < row, c, 0.0)
            lower = jnp.where((slot >= row) & (slot < last), c, 0.0)
            rows.append(jnp.concatenate([upper, lower], axis=0).astype(BF16))
        weights = jnp.concatenate(rows, axis=1)
        factor = left[pl.ds(half * blocks, blocks)].reshape(blocks * 256, left.shape[2])
        acc = acc + jnp.dot(weights, factor, preferred_element_type=F32)
    samples[...] = acc
    for n in range(out.shape[0]):
        out[n] = acc.astype(BF16)


def pack(table, words):
    tiles = [
        [table[p, 8 * h : 8 * h + 8].astype(F32) for h in range(2)] for p in range(table.shape[0])
    ]
    top = jnp.abs(tiles[0][0])
    for pair in tiles:
        for tile in pair:
            top = jnp.maximum(top, jnp.abs(tile))
    top = jnp.maximum(jnp.max(top, axis=1, keepdims=True), 1e-30)
    scale = 32700.0 / top
    for p, pair in enumerate(tiles):
        upper, lower = (jnp.round(tile * scale).astype(jnp.int32) for tile in pair)
        words[p] = (upper << 16) | (lower & 0xFFFF)
    return jnp.broadcast_to(top * (1.0 / 32700.0), (8, 128))


def lookup(words, unit, idx):
    low = idx & 127
    bit = [((idx >> (7 + n)) & 1) == 1 for n in range(5)]

    def tree(level, number):
        if level < 0:
            piece, half = number >> 1, number & 1
            source = words[piece, :, 128 * half : 128 * half + 128]
            return jnp.take_along_axis(source, low, axis=1, mode="promise_in_bounds")
        return jnp.where(bit[level], tree(level - 1, number | (1 << level)), tree(level - 1, number))

    word = tree(3, 0)
    return (jnp.where(bit[4], word << 16, word) >> 16).astype(F32) * unit


def own_kernel(table, first, partner, out, words):
    unit = pack(table, words)

    def step(n, carry):
        at = pl.multiple_of(n * 128, 128)
        a = jnp.broadcast_to(first[:, pl.ds(at, 128)], (8, 128))
        b = jnp.broadcast_to(partner[:, pl.ds(at, 128)], (8, 128))
        other = jnp.where(b >= 4096, lookup(words, unit, b), 0.0)
        out[:, pl.ds(at, 128)] = lookup(words, unit, a) - other
        return carry

    lax.fori_loop(0, first.shape[1] // 128, step, 0, unroll=8)


def emit_kernel(samples, out):
    for h in range(2):
        for s in range(8):
            out[s, h] = samples[8 * h + s : 8 * h + s + 1]


def put_rows(out, rows):
    for n in range(out.shape[0]):
        for i in range(9):
            out[n, :, 128 * i : 128 * i + 128] = rows[i]


def bin_kernel(prev, partner, base, onehot, counts, out, words, pieces):
    unit = pack(prev, words)

    def step(n, carry):
        at = pl.multiple_of(n * 128, 128)
        b = jnp.broadcast_to(partner[:, pl.ds(at, 128)], (8, 128))
        differ = base[:, pl.ds(at, 128)] - jnp.where(b < 4096, lookup(words, unit, b), 0.0)
        value = 0.5 * differ * differ
        top = value.astype(BF16).astype(F32)
        pieces[:, pl.ds(at, 128)] = jnp.concatenate([top, value - top], axis=0).astype(BF16)
        return carry

    lax.fori_loop(0, partner.shape[1] // 128, step, 0, unroll=8)
    total = nt_dot(pieces[...], onehot[...])
    sums = total[:8] + total[8:]
    put_rows(out, [sums[i : i + 1] for i in range(8)] + [counts[:1]])


def added(parts):
    total = parts[0]
    for n in range(1, parts.shape[0]):
        total = total + parts[n]
    return [total[:, 128 * i : 128 * i + 128] for i in range(9)]


def merge_kernel(parts, out):
    put_rows(out, added(parts))


def finish_kernel(parts, out):
    rows = added(parts)
    out[...] = jnp.concatenate(rows[:8], axis=0) / jnp.maximum(rows[8], 1.0)


def vmem(shape, dtype):
    return pltpu.VMEM(shape, dtype)


def body(
    noise, diag_factor, left_factor, right_factor, tile_ranks, pair_first, pair_partner, bin_ids
):
    rows = lax.axis_size(ROW)
    cols = lax.axis_size(COL)
    span = noise.shape[3]
    swap = [(0, 1), (1, 0)]
    first, partner, bins = pair_first[0], pair_partner[0], bin_ids[0]
    pairs = first.shape[1]

    local, spread_noise = call(
        copies_kernel,
        (vmem((16, span), BF16), vmem((rows, 16, span), BF16)),
        [HB],
        scratch_shapes=[pltpu.VMEM((8, 2, span), BF16), pltpu.SemaphoreType.DMA(())],
        name="copies",
    )(jnp.transpose(noise, (0, 2, 1, 3))[:, 0])
    columns = exchange(spread_noise, ROW)
    onehot, allowed, counts = call(
        prepare_kernel,
        (vmem((NBIN, pairs), BF16), vmem((8, 1, 256), F32), vmem((8, NBIN), F32)),
        [VM, SM],
        flops=1 << 20,
        name="prepare",
    )(bins, tile_ranks)
    other_noise = lax.ppermute(local, "col_1", swap)
    right = right_factor[0]

    def project(away, name):
        return call(
            functools.partial(project_kernel, away=away),
            vmem((8, 8, 256), F32),
            [VM, HB],
            flops=1 << 28,
            scratch_shapes=[pltpu.VMEM((8, 4, 64, span), BF16), pltpu.SemaphoreType.DMA((8,))],
            name=name,
        )(columns, right)

    send = project(True, "send")
    received = lax.ppermute(send, "col_1", swap)
    keep = project(False, "keep")
    pair = keep + received
    noises = call(order_kernel, vmem((32, span), BF16), [VM, VM], name="order")(local, other_noise)
    noises16 = (noises.astype(F32) * NOISE_UNIT).astype(F16)
    payload = jnp.concatenate([(pair * SUM_UNIT).astype(F16).reshape(64, 256), noises16])
    arrived = []
    for turn in TURNS:
        arrived.append(
            lax.ppermute(payload, "col_0", [(chip, (chip + turn) % 4) for chip in range(4)])
        )
    total = sum(x[:64].astype(F32) for x in arrived).reshape(8, 8, 256) * (1.0 / SUM_UNIT) + pair
    mine = jnp.where(allowed > 0.5, total, 0.0).astype(BF16)
    all_noise = [noises] + [(x[64:].astype(F32) * (1.0 / NOISE_UNIT)).astype(BF16) for x in arrived]
    theirs = lax.ppermute(mine, "col_1", swap)
    on_diag = call(
        on_diag_kernel, vmem((16, span), F32), [VM] * 5, flops=1 << 28, name="ondiag"
    )(*all_noise, diag_factor[:, 0])
    copies, own_samples = call(
        sample_kernel,
        (vmem((cols, 16, span), BF16), vmem((16, span), F32)),
        [VM, VM, VM, VM],
        flops=1 << 26,
        name="samples",
    )(mine, theirs, left_factor[0].reshape(16, 256, span), on_diag)
    own_tiles = exchange(copies, COL)
    prev_tiles = lax.ppermute(own_tiles, ROW, [(source, source + 1) for source in range(rows - 1)])
    samples = call(
        emit_kernel, jax.ShapeDtypeStruct((8, 2, 1, span), F32), [VM], name="emit"
    )(own_samples)
    base = call(
        own_kernel,
        vmem((8, pairs), F32),
        [VM, VM, VM],
        flops=1 << 26,
        scratch_shapes=[pltpu.VMEM((cols, 8, span), jnp.int32)],
        name="own",
    )(own_tiles, first, partner)
    partial = call(
        bin_kernel,
        vmem((lax.axis_size(ZC), 1, 9 * NBIN), F32),
        [VM, VM, VM, VM, VM],
        flops=1 << 26,
        scratch_shapes=[
            pltpu.VMEM((cols, 8, span), jnp.int32),
            pltpu.VMEM((16, pairs), BF16),
        ],
        name="bins",
    )(prev_tiles, partner, base, onehot, counts)
    merged = call(merge_kernel, vmem((lax.axis_size(XY), 1, 9 * NBIN), F32), [VM], name="merge")(
        exchange(partial, ZC)
    )
    variogram = call(finish_kernel, jax.ShapeDtypeStruct((8, NBIN), F32), [VM], name="finish")(exchange(merged, XY))
    return (samples, variogram)


def solution(mesh):
    split = Mesh(mesh.devices.reshape(4, 2, 4, 4, 2), ("row_0", "row_1", "row_2", "col_0", "col_1"))
    return jax.shard_map(
        body,
        mesh=split,
        in_specs=(
            P(None, None, ROW, COL),
            P(None, ROW, COL, None),
            P(ROW, None, None, COL),
            P(ROW, None, None, COL),
            P(ROW, None),
            P(ROW, COL, None),
            P(ROW, COL, None),
            P(ROW, COL, None),
        ),
        out_specs=(P(None, None, ROW, COL), P()),
        check_vma=False,
    )
```

```python
import functools

import jax
import jax.numpy as jnp
from jax import lax
from jax.experimental import pallas as pl
from jax.experimental.pallas import tpu as pltpu
from jax.sharding import Mesh
from jax.sharding import PartitionSpec as P

NBIN = 128
ROW = ("row_0", "row_1", "row_2")
COL = ("col_0", "col_1")
XY = ("row_0", "row_2")
ZC = ("row_1", "col_0", "col_1")
F32 = jnp.float32
F16 = jnp.float16
SUM_UNIT = 128.0
NOISE_UNIT = 1024.0
TURNS = (2, 1, 3)
BF16 = jnp.bfloat16


def exchange(copies, axis):
    return lax.all_to_all(copies, axis, 0, 0, tiled=True)


def nt_dot(a, b):
    return lax.dot_general(a, b, (((1,), (1,)), ((), ())), preferred_element_type=F32)


HB = pl.BlockSpec(memory_space=pltpu.HBM)
VM = pl.BlockSpec(memory_space=pltpu.VMEM)
SM = pl.BlockSpec(memory_space=pltpu.SMEM)


def call(kernel, out_shape, in_specs, flops=1, **kw):
    run = pl.pallas_call(
        kernel,
        out_shape=out_shape,
        in_specs=in_specs,
        cost_estimate=pl.CostEstimate(flops=flops, bytes_accessed=1 << 20, transcendentals=0),
        compiler_params=pltpu.CompilerParams(vmem_limit_bytes=16 << 20),
        **kw,
    )

    def held(*args):
        return run(
            *(
                a if spec is SM else pltpu.with_memory_space_constraint(a, spec.memory_space)
                for a, spec in zip(args, in_specs)
            )
        )

    return held


def copies_kernel(source, factor, local, out, right, noise, sems):
    copy = pltpu.make_async_copy(source, noise, sems.at[0])
    fetch = pltpu.make_async_copy(factor, right, sems.at[1])
    copy.start()
    fetch.start()
    copy.wait()
    rows = [noise[s].astype(F32)[h : h + 1] for h in range(2) for s in range(8)]
    mine = jnp.concatenate(rows, axis=0).astype(BF16)
    local[...] = mine
    for n in range(out.shape[0]):
        out[n] = mine
    fetch.wait()


def prepare_kernel(bins, ranks, onehot, keep, counts):
    core = lax.axis_index("col_1")
    lane = lax.broadcasted_iota(jnp.int32, (1, 256), 1)
    for i in range(keep.shape[0]):
        slot = 4 * (core * keep.shape[0] + i)
        limit = ranks[0, slot + 3] + 192
        for n in (2, 1, 0):
            limit = jnp.where(lane < 64 * n + 64, ranks[0, slot + n] + 64 * n, limit)
        keep[i] = jnp.where(lane < limit, 1.0, 0.0)
    bin_at = lax.broadcasted_iota(jnp.int32, (NBIN, 128), 0)

    def step(n, carry):
        at = pl.multiple_of(n * 128, 128)
        ids = jnp.broadcast_to(bins[:, pl.ds(at, 128)], (NBIN, 128))
        onehot[:, pl.ds(at, 128)] = jnp.where(ids == bin_at, 1.0, 0.0).astype(BF16)
        return carry

    lax.fori_loop(0, bins.shape[1] // 128, step, 0, unroll=4)
    counts[...] = nt_dot(jnp.ones((8, onehot.shape[1]), BF16), onehot[...])


def order_kernel(local, other, out):
    first = lax.axis_index("col_1") == 0
    own = local[...].astype(F32)
    far = other[...].astype(F32)
    out[:16] = jnp.where(first, own, far).astype(BF16)
    out[16:] = jnp.where(first, far, own).astype(BF16)


def project_kernel(columns, right, out, *, away):
    row, core = lax.axis_index(ROW), lax.axis_index("col_1")
    half = 1 - core if away else core
    tiles = 2 * columns.shape[0]
    groups = right.shape[0] // 8
    lane = lax.broadcasted_iota(jnp.int32, (8, 128), 1)

    def step(g, carry):
        base = (half * groups + g) * 4
        blocks = []
        low = []
        for n in range(4):
            slot = base + n
            tile = jnp.where(slot < row, slot, slot - row)
            first = tile < tiles // 2
            blocks.append(columns[jnp.where(first, tile, tiles - 1 - tile)])
            low.append(first)
        factor = right[pl.ds(base, 4)].reshape(256, 256)
        full = nt_dot(jnp.concatenate(blocks, axis=0), factor)
        parts = []
        for n in range(4):
            cols = full[16 * n : 16 * n + 16, 128 * (n // 2) : 128 * (n // 2) + 128]
            parts.append(jnp.where(low[n], cols[:8], cols[8:]))
        out[g, :, :128] = jnp.where(lane < 64, parts[0], parts[1])
        out[g, :, 128:] = jnp.where(lane < 64, parts[2], parts[3])
        return carry

    lax.fori_loop(0, groups, step, 0, unroll=4)


def on_diag_kernel(n0, n1, n2, n3, diag, out):
    col, chip = lax.axis_index(COL), lax.axis_index("col_0")
    span = diag.shape[1]
    own = jnp.where(lax.axis_index("col_1") == 0, n0[:16].astype(F32), n0[16:].astype(F32))
    i_at = lax.broadcasted_iota(jnp.int32, (span, span), 0)
    j_at = lax.broadcasted_iota(jnp.int32, (span, span), 1)
    acc = [own, own]
    at = pl.multiple_of(col * span, span)
    for h in range(2):
        corner = jnp.where(j_at < i_at, diag[h, :, pl.ds(at, span)].astype(F32), 0.0).astype(BF16)
        acc[h] = acc[h] + nt_dot(own.astype(BF16), corner)
    for noise, turn in zip((n0, n1, n2, n3), (0, *TURNS)):
        for core in range(2):
            number = 2 * lax.rem(chip + 4 - turn, 4) + core
            piece = noise[16 * core : 16 * core + 16].astype(F32)
            piece = jnp.where(number < col, piece, 0.0).astype(BF16)
            from_ = pl.multiple_of(number * span, span)
            for h in range(2):
                acc[h] = acc[h] + nt_dot(piece, diag[h, :, pl.ds(from_, span)])
    for h in range(2):
        out[8 * h : 8 * h + 8] = acc[h][8 * h : 8 * h + 8]


def sample_kernel(mine, theirs, left, on_diag, out, samples):
    row, core = lax.axis_index(ROW), lax.axis_index("col_1")
    blocks = mine.shape[0]
    last = 8 * blocks - 1
    side = lax.broadcasted_iota(jnp.int32, (8, 256), 1) >> 6
    acc = on_diag[...]
    for half, coeffs in ((core, mine), (1 - core, theirs)):
        rows = []
        for i in range(blocks):
            slot = 4 * (half * blocks + i) + side
            c = coeffs[i].astype(F32)
            upper = jnp.where(slot < row, c, 0.0)
            lower = jnp.where((slot >= row) & (slot < last), c, 0.0)
            rows.append(jnp.concatenate([upper, lower], axis=0).astype(BF16))
        weights = jnp.concatenate(rows, axis=1)
        factor = left[pl.ds(half * blocks, blocks)].reshape(blocks * 256, left.shape[2])
        acc = acc + jnp.dot(weights, factor, preferred_element_type=F32)
    samples[...] = acc
    for n in range(out.shape[0]):
        out[n] = acc.astype(BF16)


def pack(table, words):
    tiles = [
        [table[p, 8 * h : 8 * h + 8].astype(F32) for h in range(2)] for p in range(table.shape[0])
    ]
    top = jnp.abs(tiles[0][0])
    for pair in tiles:
        for tile in pair:
            top = jnp.maximum(top, jnp.abs(tile))
    top = jnp.maximum(jnp.max(top, axis=1, keepdims=True), 1e-30)
    scale = 32700.0 / top
    for p, pair in enumerate(tiles):
        upper, lower = (jnp.round(tile * scale).astype(jnp.int32) for tile in pair)
        words[p] = (upper << 16) | (lower & 0xFFFF)
    return jnp.broadcast_to(top * (1.0 / 32700.0), (8, 128))


def lookup(words, unit, idx):
    low = idx & 127
    bit = [((idx >> (7 + n)) & 1) == 1 for n in range(5)]

    def tree(level, number):
        if level < 0:
            piece, half = number >> 1, number & 1
            source = words[piece, :, 128 * half : 128 * half + 128]
            return jnp.take_along_axis(source, low, axis=1, mode="promise_in_bounds")
        return jnp.where(bit[level], tree(level - 1, number | (1 << level)), tree(level - 1, number))

    word = tree(3, 0)
    return (jnp.where(bit[4], word << 16, word) >> 16).astype(F32) * unit


def own_kernel(table, first, partner, out, words):
    unit = pack(table, words)

    def step(n, carry):
        at = pl.multiple_of(n * 128, 128)
        a = jnp.broadcast_to(first[:, pl.ds(at, 128)], (8, 128))
        b = jnp.broadcast_to(partner[:, pl.ds(at, 128)], (8, 128))
        other = jnp.where(b >= 4096, lookup(words, unit, b), 0.0)
        out[:, pl.ds(at, 128)] = lookup(words, unit, a) - other
        return carry

    lax.fori_loop(0, first.shape[1] // 128, step, 0, unroll=8)


def emit_kernel(samples, out):
    for h in range(2):
        for s in range(8):
            out[s, h] = samples[8 * h + s : 8 * h + s + 1]


def put_rows(out, rows):
    for n in range(out.shape[0]):
        for i in range(9):
            out[n, :, 128 * i : 128 * i + 128] = rows[i]


def bin_kernel(prev, partner, base, onehot, counts, out, words, pieces):
    unit = pack(prev, words)

    def step(n, carry):
        at = pl.multiple_of(n * 128, 128)
        b = jnp.broadcast_to(partner[:, pl.ds(at, 128)], (8, 128))
        differ = base[:, pl.ds(at, 128)] - jnp.where(b < 4096, lookup(words, unit, b), 0.0)
        value = 0.5 * differ * differ
        top = value.astype(BF16).astype(F32)
        pieces[:, pl.ds(at, 128)] = jnp.concatenate([top, value - top], axis=0).astype(BF16)
        return carry

    lax.fori_loop(0, partner.shape[1] // 128, step, 0, unroll=8)
    total = nt_dot(pieces[...], onehot[...])
    sums = total[:8] + total[8:]
    put_rows(out, [sums[i : i + 1] for i in range(8)] + [counts[:1]])


def added(parts):
    total = parts[0]
    for n in range(1, parts.shape[0]):
        total = total + parts[n]
    return [total[:, 128 * i : 128 * i + 128] for i in range(9)]


def merge_kernel(parts, out):
    put_rows(out, added(parts))


def finish_kernel(parts, out):
    rows = added(parts)
    out[...] = jnp.concatenate(rows[:8], axis=0) / jnp.maximum(rows[8], 1.0)


def vmem(shape, dtype):
    return pltpu.VMEM(shape, dtype)


def body(
    noise, diag_factor, left_factor, right_factor, tile_ranks, pair_first, pair_partner, bin_ids
):
    rows = lax.axis_size(ROW)
    cols = lax.axis_size(COL)
    span = noise.shape[3]
    swap = [(0, 1), (1, 0)]
    first, partner, bins = pair_first[0], pair_partner[0], bin_ids[0]
    pairs = first.shape[1]

    local, spread_noise, right = call(
        copies_kernel,
        (
            vmem((16, span), BF16),
            vmem((rows, 16, span), BF16),
            vmem(right_factor.shape[1:], BF16),
        ),
        [HB, HB],
        scratch_shapes=[pltpu.VMEM((8, 2, span), BF16), pltpu.SemaphoreType.DMA((2,))],
        name="copies",
    )(jnp.transpose(noise, (0, 2, 1, 3))[:, 0], right_factor[0])
    columns = exchange(spread_noise, ROW)
    onehot, allowed, counts = call(
        prepare_kernel,
        (vmem((NBIN, pairs), BF16), vmem((8, 1, 256), F32), vmem((8, NBIN), F32)),
        [VM, SM],
        flops=1 << 20,
        name="prepare",
    )(bins, tile_ranks)
    other_noise = lax.ppermute(local, "col_1", swap)

    def project(away, name):
        return call(
            functools.partial(project_kernel, away=away),
            vmem((8, 8, 256), F32),
            [VM, VM],
            flops=1 << 28,
            name=name,
        )(columns, right)

    send = project(True, "send")
    received = lax.ppermute(send, "col_1", swap)
    keep = project(False, "keep")
    pair = keep + received
    noises = call(order_kernel, vmem((32, span), BF16), [VM, VM], name="order")(local, other_noise)
    noises16 = (noises.astype(F32) * NOISE_UNIT).astype(F16)
    payload = jnp.concatenate([(pair * SUM_UNIT).astype(F16).reshape(64, 256), noises16])
    arrived = []
    for turn in TURNS:
        arrived.append(
            lax.ppermute(payload, "col_0", [(chip, (chip + turn) % 4) for chip in range(4)])
        )
    total = sum(x[:64].astype(F32) for x in arrived).reshape(8, 8, 256) * (1.0 / SUM_UNIT) + pair
    mine = jnp.where(allowed > 0.5, total, 0.0).astype(BF16)
    all_noise = [noises] + [(x[64:].astype(F32) * (1.0 / NOISE_UNIT)).astype(BF16) for x in arrived]
    theirs = lax.ppermute(mine, "col_1", swap)
    on_diag = call(
        on_diag_kernel, vmem((16, span), F32), [VM] * 5, flops=1 << 28, name="ondiag"
    )(*all_noise, diag_factor[:, 0])
    copies, own_samples = call(
        sample_kernel,
        (vmem((cols, 16, span), BF16), vmem((16, span), F32)),
        [VM, VM, VM, VM],
        flops=1 << 26,
        name="samples",
    )(mine, theirs, left_factor[0].reshape(16, 256, span), on_diag)
    own_tiles = exchange(copies, COL)
    prev_tiles = lax.ppermute(own_tiles, ROW, [(source, source + 1) for source in range(rows - 1)])
    samples = call(
        emit_kernel, jax.ShapeDtypeStruct((8, 2, 1, span), F32), [VM], name="emit"
    )(own_samples)
    base = call(
        own_kernel,
        vmem((8, pairs), F32),
        [VM, VM, VM],
        flops=1 << 26,
        scratch_shapes=[pltpu.VMEM((cols, 8, span), jnp.int32)],
        name="own",
    )(own_tiles, first, partner)
    partial = call(
        bin_kernel,
        vmem((lax.axis_size(ZC), 1, 9 * NBIN), F32),
        [VM, VM, VM, VM, VM],
        flops=1 << 26,
        scratch_shapes=[
            pltpu.VMEM((cols, 8, span), jnp.int32),
            pltpu.VMEM((16, pairs), BF16),
        ],
        name="bins",
    )(prev_tiles, partner, base, onehot, counts)
    merged = call(merge_kernel, vmem((lax.axis_size(XY), 1, 9 * NBIN), F32), [VM], name="merge")(
        exchange(partial, ZC)
    )
    variogram = call(finish_kernel, jax.ShapeDtypeStruct((8, NBIN), F32), [VM], name="finish")(exchange(merged, XY))
    return (samples, variogram)


def solution(mesh):
    split = Mesh(mesh.devices.reshape(4, 2, 4, 4, 2), ("row_0", "row_1", "row_2", "col_0", "col_1"))
    return jax.shard_map(
        body,
        mesh=split,
        in_specs=(
            P(None, None, ROW, COL),
            P(None, ROW, COL, None),
            P(ROW, None, None, COL),
            P(ROW, None, None, COL),
            P(ROW, None),
            P(ROW, COL, None),
            P(ROW, COL, None),
            P(ROW, COL, None),
        ),
        out_specs=(P(None, None, ROW, COL), P()),
        check_vma=False,
    )
```

```python
import functools

import jax
import jax.numpy as jnp
from jax import lax
from jax.experimental import pallas as pl
from jax.experimental.pallas import tpu as pltpu
from jax.sharding import Mesh
from jax.sharding import PartitionSpec as P

NBIN = 128
ROW = ("row_0", "row_1", "row_2")
COL = ("col_0", "col_1")
XY = ("row_0", "row_2")
ZC = ("row_1", "col_0", "col_1")
F32 = jnp.float32
F16 = jnp.float16
SUM_UNIT = 128.0
NOISE_UNIT = 1024.0
TURNS = (2, 1, 3)
BF16 = jnp.bfloat16


def exchange(copies, axis):
    return lax.all_to_all(copies, axis, 0, 0, tiled=True)


def nt_dot(a, b):
    return lax.dot_general(a, b, (((1,), (1,)), ((), ())), preferred_element_type=F32)


HB = pl.BlockSpec(memory_space=pltpu.HBM)
VM = pl.BlockSpec(memory_space=pltpu.VMEM)
SM = pl.BlockSpec(memory_space=pltpu.SMEM)


def call(kernel, out_shape, in_specs, flops=1, **kw):
    run = pl.pallas_call(
        kernel,
        out_shape=out_shape,
        in_specs=in_specs,
        cost_estimate=pl.CostEstimate(flops=flops, bytes_accessed=1 << 20, transcendentals=0),
        compiler_params=pltpu.CompilerParams(vmem_limit_bytes=16 << 20),
        **kw,
    )

    def held(*args):
        return run(
            *(
                a if spec is SM else pltpu.with_memory_space_constraint(a, spec.memory_space)
                for a, spec in zip(args, in_specs)
            )
        )

    return held


def copies_kernel(source, factor, local, out, right, noise, sems):
    copy = pltpu.make_async_copy(source, noise, sems.at[0])
    half = right.shape[0]
    away = (1 - lax.axis_index("col_1")) * half
    fetch = pltpu.make_async_copy(factor.at[pl.ds(away, half)], right, sems.at[1])
    copy.start()
    fetch.start()
    copy.wait()
    rows = [noise[s].astype(F32)[h : h + 1] for h in range(2) for s in range(8)]
    mine = jnp.concatenate(rows, axis=0).astype(BF16)
    local[...] = mine
    for n in range(out.shape[0]):
        out[n] = mine
    fetch.wait()


def prepare_kernel(bins, ranks, onehot, keep, counts):
    core = lax.axis_index("col_1")
    lane = lax.broadcasted_iota(jnp.int32, (1, 256), 1)
    for i in range(keep.shape[0]):
        slot = 4 * (core * keep.shape[0] + i)
        limit = ranks[0, slot + 3] + 192
        for n in (2, 1, 0):
            limit = jnp.where(lane < 64 * n + 64, ranks[0, slot + n] + 64 * n, limit)
        keep[i] = jnp.where(lane < limit, 1.0, 0.0)
    bin_at = lax.broadcasted_iota(jnp.int32, (NBIN, 128), 0)

    def step(n, carry):
        at = pl.multiple_of(n * 128, 128)
        ids = jnp.broadcast_to(bins[:, pl.ds(at, 128)], (NBIN, 128))
        onehot[:, pl.ds(at, 128)] = jnp.where(ids == bin_at, 1.0, 0.0).astype(BF16)
        return carry

    lax.fori_loop(0, bins.shape[1] // 128, step, 0, unroll=4)
    counts[...] = nt_dot(jnp.ones((8, onehot.shape[1]), BF16), onehot[...])


def payload_kernel(keep, received, local, other, out):
    for g in range(keep.shape[0]):
        out[8 * g : 8 * g + 8] = (keep[g] + received[g]) * SUM_UNIT
    out[64:80] = local[...].astype(F32) * NOISE_UNIT
    out[80:] = other[...].astype(F32) * NOISE_UNIT


def project_kernel(columns, right, out, *, away):
    row, core = lax.axis_index(ROW), lax.axis_index("col_1")
    half = 1 - core if away else core
    tiles = 2 * columns.shape[0]
    groups = out.shape[0]
    lane = lax.broadcasted_iota(jnp.int32, (8, 128), 1)

    def step(g, carry):
        base = (half * groups + g) * 4
        at = 4 * g if away else base
        blocks = []
        low = []
        for n in range(4):
            slot = base + n
            tile = jnp.where(slot < row, slot, slot - row)
            first = tile < tiles // 2
            blocks.append(columns[jnp.where(first, tile, tiles - 1 - tile)])
            low.append(first)
        factor = right[pl.ds(at, 4)].reshape(256, 256)
        full = nt_dot(jnp.concatenate(blocks, axis=0), factor)
        parts = []
        for n in range(4):
            cols = full[16 * n : 16 * n + 16, 128 * (n // 2) : 128 * (n // 2) + 128]
            parts.append(jnp.where(low[n], cols[:8], cols[8:]))
        out[g, :, :128] = jnp.where(lane < 64, parts[0], parts[1])
        out[g, :, 128:] = jnp.where(lane < 64, parts[2], parts[3])
        return carry

    lax.fori_loop(0, groups, step, 0, unroll=4)


def on_diag_kernel(local, other, n1, n2, n3, diag, out):
    col, chip, mine = lax.axis_index(COL), lax.axis_index("col_0"), lax.axis_index("col_1")
    span = diag.shape[1]
    own = local[...].astype(F32)
    i_at = lax.broadcasted_iota(jnp.int32, (span, span), 0)
    j_at = lax.broadcasted_iota(jnp.int32, (span, span), 1)
    acc = [own, own]
    at = pl.multiple_of(col * span, span)
    for h in range(2):
        corner = jnp.where(j_at < i_at, diag[h, :, pl.ds(at, span)].astype(F32), 0.0).astype(BF16)
        acc[h] = acc[h] + nt_dot(own.astype(BF16), corner)
    near = ((local, 0), (other, 0))
    for turn, places in zip(
        (0, *TURNS), (near, ((n1, 0), (n1, 16)), ((n2, 0), (n2, 16)), ((n3, 0), (n3, 16)))
    ):
        for core, (noise, row) in zip((mine, 1 - mine), places):
            number = 2 * lax.rem(chip + 4 - turn, 4) + core
            piece = noise[row : row + 16].astype(F32)
            piece = jnp.where(number < col, piece, 0.0).astype(BF16)
            from_ = pl.multiple_of(number * span, span)
            for h in range(2):
                acc[h] = acc[h] + nt_dot(piece, diag[h, :, pl.ds(from_, span)])
    for h in range(2):
        out[8 * h : 8 * h + 8] = acc[h][8 * h : 8 * h + 8]


def sample_kernel(mine, theirs, left, on_diag, out, samples):
    row, core = lax.axis_index(ROW), lax.axis_index("col_1")
    blocks = mine.shape[0]
    last = 8 * blocks - 1
    side = lax.broadcasted_iota(jnp.int32, (8, 256), 1) >> 6
    acc = on_diag[...]
    for half, coeffs in ((core, mine), (1 - core, theirs)):
        rows = []
        for i in range(blocks):
            slot = 4 * (half * blocks + i) + side
            c = coeffs[i].astype(F32)
            upper = jnp.where(slot < row, c, 0.0)
            lower = jnp.where((slot >= row) & (slot < last), c, 0.0)
            rows.append(jnp.concatenate([upper, lower], axis=0).astype(BF16))
        weights = jnp.concatenate(rows, axis=1)
        factor = left[pl.ds(half * blocks, blocks)].reshape(blocks * 256, left.shape[2])
        acc = acc + jnp.dot(weights, factor, preferred_element_type=F32)
    samples[...] = acc
    for n in range(out.shape[0]):
        out[n] = acc.astype(BF16)


def pack(table, words):
    tiles = [
        [table[p, 8 * h : 8 * h + 8].astype(F32) for h in range(2)] for p in range(table.shape[0])
    ]
    top = jnp.abs(tiles[0][0])
    for pair in tiles:
        for tile in pair:
            top = jnp.maximum(top, jnp.abs(tile))
    top = jnp.maximum(jnp.max(top, axis=1, keepdims=True), 1e-30)
    scale = 32700.0 / top
    for p, pair in enumerate(tiles):
        upper, lower = (jnp.round(tile * scale).astype(jnp.int32) for tile in pair)
        words[p] = (upper << 16) | (lower & 0xFFFF)
    return jnp.broadcast_to(top * (1.0 / 32700.0), (8, 128))


def lookup(words, unit, idx):
    low = idx & 127
    bit = [((idx >> (7 + n)) & 1) == 1 for n in range(5)]

    def tree(level, number):
        if level < 0:
            piece, half = number >> 1, number & 1
            source = words[piece, :, 128 * half : 128 * half + 128]
            return jnp.take_along_axis(source, low, axis=1, mode="promise_in_bounds")
        return jnp.where(bit[level], tree(level - 1, number | (1 << level)), tree(level - 1, number))

    word = tree(3, 0)
    return (jnp.where(bit[4], word << 16, word) >> 16).astype(F32) * unit


def own_kernel(table, first, partner, out, words):
    unit = pack(table, words)

    def step(n, carry):
        at = pl.multiple_of(n * 128, 128)
        a = jnp.broadcast_to(first[:, pl.ds(at, 128)], (8, 128))
        b = jnp.broadcast_to(partner[:, pl.ds(at, 128)], (8, 128))
        other = jnp.where(b >= 4096, lookup(words, unit, b), 0.0)
        out[:, pl.ds(at, 128)] = lookup(words, unit, a) - other
        return carry

    lax.fori_loop(0, first.shape[1] // 128, step, 0, unroll=16)


def emit_kernel(samples, out):
    for h in range(2):
        for s in range(8):
            out[s, h] = samples[8 * h + s : 8 * h + s + 1]


def put_rows(out, rows):
    for n in range(out.shape[0]):
        for i in range(9):
            out[n, :, 128 * i : 128 * i + 128] = rows[i]


def bin_kernel(prev, partner, base, onehot, counts, out, words, pieces):
    unit = pack(prev, words)

    def step(n, carry):
        at = pl.multiple_of(n * 128, 128)
        b = jnp.broadcast_to(partner[:, pl.ds(at, 128)], (8, 128))
        differ = base[:, pl.ds(at, 128)] - jnp.where(b < 4096, lookup(words, unit, b), 0.0)
        value = 0.5 * differ * differ
        top = value.astype(BF16).astype(F32)
        pieces[:, pl.ds(at, 128)] = jnp.concatenate([top, value - top], axis=0).astype(BF16)
        return carry

    lax.fori_loop(0, partner.shape[1] // 128, step, 0, unroll=16)
    total = nt_dot(pieces[...], onehot[...])
    sums = total[:8] + total[8:]
    put_rows(out, [sums[i : i + 1] for i in range(8)] + [counts[:1]])


def added(parts):
    total = parts[0]
    for n in range(1, parts.shape[0]):
        total = total + parts[n]
    return [total[:, 128 * i : 128 * i + 128] for i in range(9)]


def merge_kernel(parts, out):
    put_rows(out, added(parts))


def finish_kernel(parts, out):
    rows = added(parts)
    out[...] = jnp.concatenate(rows[:8], axis=0) / jnp.maximum(rows[8], 1.0)


def vmem(shape, dtype):
    return pltpu.VMEM(shape, dtype)


def body(
    noise, diag_factor, left_factor, right_factor, tile_ranks, pair_first, pair_partner, bin_ids
):
    rows = lax.axis_size(ROW)
    cols = lax.axis_size(COL)
    span = noise.shape[3]
    swap = [(0, 1), (1, 0)]
    first, partner, bins = pair_first[0], pair_partner[0], bin_ids[0]
    pairs = first.shape[1]

    local, spread_noise, right_away = call(
        copies_kernel,
        (
            vmem((16, span), BF16),
            vmem((rows, 16, span), BF16),
            vmem((32, 64, span), BF16),
        ),
        [HB, HB],
        scratch_shapes=[pltpu.VMEM((8, 2, span), BF16), pltpu.SemaphoreType.DMA((2,))],
        name="copies",
    )(jnp.transpose(noise, (0, 2, 1, 3))[:, 0], right_factor[0])
    columns = exchange(spread_noise, ROW)
    onehot, allowed, counts = call(
        prepare_kernel,
        (vmem((NBIN, pairs), BF16), vmem((8, 1, 256), F32), vmem((8, NBIN), F32)),
        [VM, SM],
        flops=1 << 20,
        name="prepare",
    )(bins, tile_ranks)
    other_noise = lax.ppermute(local, "col_1", swap)

    def project(away, name):
        return call(
            functools.partial(project_kernel, away=away),
            vmem((8, 8, 256), F32),
            [VM, VM],
            flops=1 << 28,
            name=name,
        )(columns, right_away if away else right_factor[0])

    send = project(True, "send")
    received = lax.ppermute(send, "col_1", swap)
    keep = project(False, "keep")
    payload = call(payload_kernel, vmem((96, span), F32), [VM] * 4, name="payload")(
        keep, received, local, other_noise
    ).astype(F16)
    arrived = []
    for turn in TURNS:
        arrived.append(
            lax.ppermute(payload, "col_0", [(chip, (chip + turn) % 4) for chip in range(4)])
        )
    total = sum(x[:64].astype(F32) for x in arrived).reshape(8, 8, span) * (1.0 / SUM_UNIT)
    total = (total + keep) + received
    mine = jnp.where(allowed > 0.5, total, 0.0).astype(BF16)
    all_noise = [
        (x[64:].astype(F32) * (1.0 / NOISE_UNIT)).astype(BF16) for x in arrived
    ]
    theirs = lax.ppermute(mine, "col_1", swap)
    on_diag = call(
        on_diag_kernel, vmem((16, span), F32), [VM] * 6, flops=1 << 28, name="ondiag"
    )(local, other_noise, *all_noise, diag_factor[:, 0])
    copies, own_samples = call(
        sample_kernel,
        (vmem((cols, 16, span), BF16), vmem((16, span), F32)),
        [VM, VM, VM, VM],
        flops=1 << 26,
        name="samples",
    )(mine, theirs, left_factor[0].reshape(16, 256, span), on_diag)
    own_tiles = exchange(copies, COL)
    prev_tiles = lax.ppermute(own_tiles, ROW, [(source, source + 1) for source in range(rows - 1)])
    samples = call(
        emit_kernel, jax.ShapeDtypeStruct((8, 2, 1, span), F32), [VM], name="emit"
    )(own_samples)
    base = call(
        own_kernel,
        vmem((8, pairs), F32),
        [VM, VM, VM],
        flops=1 << 26,
        scratch_shapes=[pltpu.VMEM((cols, 8, span), jnp.int32)],
        name="own",
    )(own_tiles, first, partner)
    partial = call(
        bin_kernel,
        vmem((lax.axis_size(ZC), 1, 9 * NBIN), F32),
        [VM, VM, VM, VM, VM],
        flops=1 << 26,
        scratch_shapes=[
            pltpu.VMEM((cols, 8, span), jnp.int32),
            pltpu.VMEM((16, pairs), BF16),
        ],
        name="bins",
    )(prev_tiles, partner, base, onehot, counts)
    merged = call(merge_kernel, vmem((lax.axis_size(XY), 1, 9 * NBIN), F32), [VM], name="merge")(
        exchange(partial, ZC)
    )
    variogram = call(finish_kernel, jax.ShapeDtypeStruct((8, NBIN), F32), [VM], name="finish")(exchange(merged, XY))
    return (samples, variogram)


def solution(mesh):
    split = Mesh(mesh.devices.reshape(4, 2, 4, 4, 2), ("row_0", "row_1", "row_2", "col_0", "col_1"))
    return jax.shard_map(
        body,
        mesh=split,
        in_specs=(
            P(None, None, ROW, COL),
            P(None, ROW, COL, None),
            P(ROW, None, None, COL),
            P(ROW, None, None, COL),
            P(ROW, None),
            P(ROW, COL, None),
            P(ROW, COL, None),
            P(ROW, COL, None),
        ),
        out_specs=(P(None, None, ROW, COL), P()),
        check_vma=False,
    )
```

```python
import functools

import jax
import jax.numpy as jnp
from jax import lax
from jax.experimental import pallas as pl
from jax.experimental.pallas import tpu as pltpu
from jax.sharding import Mesh
from jax.sharding import PartitionSpec as P

NBIN = 128
ROW = ("row_0", "row_1", "row_2")
COL = ("col_0", "col_1")
XY = ("row_0", "row_2")
ZC = ("row_1", "col_0", "col_1")
F32 = jnp.float32
F16 = jnp.float16
SUM_UNIT = 128.0
NOISE_UNIT = 1024.0
TURNS = (2, 1, 3)
BF16 = jnp.bfloat16


def exchange(copies, axis):
    return lax.all_to_all(copies, axis, 0, 0, tiled=True)


def nt_dot(a, b):
    return lax.dot_general(a, b, (((1,), (1,)), ((), ())), preferred_element_type=F32)


HB = pl.BlockSpec(memory_space=pltpu.HBM)
VM = pl.BlockSpec(memory_space=pltpu.VMEM)
SM = pl.BlockSpec(memory_space=pltpu.SMEM)


def call(kernel, out_shape, in_specs, flops=1, **kw):
    run = pl.pallas_call(
        kernel,
        out_shape=out_shape,
        in_specs=in_specs,
        cost_estimate=pl.CostEstimate(flops=flops, bytes_accessed=1 << 20, transcendentals=0),
        compiler_params=pltpu.CompilerParams(vmem_limit_bytes=16 << 20),
        **kw,
    )

    def held(*args):
        return run(
            *(
                a if spec is SM else pltpu.with_memory_space_constraint(a, spec.memory_space)
                for a, spec in zip(args, in_specs)
            )
        )

    return held


def copies_kernel(source, local, out, noise, sem):
    copy = pltpu.make_async_copy(source, noise, sem)
    copy.start()
    copy.wait()
    rows = [noise[s].astype(F32)[h : h + 1] for h in range(2) for s in range(8)]
    mine = jnp.concatenate(rows, axis=0).astype(BF16)
    local[...] = mine
    for n in range(out.shape[0]):
        out[n] = mine


def prepare_kernel(bins, ranks, onehot, keep, counts):
    core = lax.axis_index("col_1")
    lane = lax.broadcasted_iota(jnp.int32, (1, 256), 1)
    for i in range(keep.shape[0]):
        slot = 4 * (core * keep.shape[0] + i)
        limit = ranks[0, slot + 3] + 192
        for n in (2, 1, 0):
            limit = jnp.where(lane < 64 * n + 64, ranks[0, slot + n] + 64 * n, limit)
        keep[i] = jnp.where(lane < limit, 1.0, 0.0)
    bin_at = lax.broadcasted_iota(jnp.int32, (NBIN, 128), 0)

    def step(n, carry):
        at = pl.multiple_of(n * 128, 128)
        ids = jnp.broadcast_to(bins[:, pl.ds(at, 128)], (NBIN, 128))
        onehot[:, pl.ds(at, 128)] = jnp.where(ids == bin_at, 1.0, 0.0).astype(BF16)
        return carry

    lax.fori_loop(0, bins.shape[1] // 128, step, 0, unroll=4)
    counts[...] = nt_dot(jnp.ones((8, onehot.shape[1]), BF16), onehot[...])


def payload_kernel(keep, received, local, other, out):
    for g in range(keep.shape[0]):
        out[8 * g : 8 * g + 8] = (keep[g] + received[g]) * SUM_UNIT
    out[64:80] = local[...].astype(F32) * NOISE_UNIT
    out[80:] = other[...].astype(F32) * NOISE_UNIT


def project_kernel(columns, right, out, *, away):
    row, core = lax.axis_index(ROW), lax.axis_index("col_1")
    half = 1 - core if away else core
    tiles = 2 * columns.shape[0]
    groups = out.shape[0]
    lane = lax.broadcasted_iota(jnp.int32, (8, 128), 1)

    def step(g, carry):
        base = (half * groups + g) * 4
        blocks = []
        low = []
        for n in range(4):
            slot = base + n
            tile = jnp.where(slot < row, slot, slot - row)
            first = tile < tiles // 2
            blocks.append(columns[jnp.where(first, tile, tiles - 1 - tile)])
            low.append(first)
        factor = right[pl.ds(base, 4)].reshape(256, 256)
        full = nt_dot(jnp.concatenate(blocks, axis=0), factor)
        parts = []
        for n in range(4):
            cols = full[16 * n : 16 * n + 16, 128 * (n // 2) : 128 * (n // 2) + 128]
            parts.append(jnp.where(low[n], cols[:8], cols[8:]))
        out[g, :, :128] = jnp.where(lane < 64, parts[0], parts[1])
        out[g, :, 128:] = jnp.where(lane < 64, parts[2], parts[3])
        return carry

    lax.fori_loop(0, groups, step, 0, unroll=4)


def on_diag_kernel(local, other, n1, n2, n3, diag, out):
    col, chip, mine = lax.axis_index(COL), lax.axis_index("col_0"), lax.axis_index("col_1")
    span = diag.shape[1]
    own = local[...].astype(F32)
    i_at = lax.broadcasted_iota(jnp.int32, (span, span), 0)
    j_at = lax.broadcasted_iota(jnp.int32, (span, span), 1)
    acc = [own, own]
    at = pl.multiple_of(col * span, span)
    for h in range(2):
        corner = jnp.where(j_at < i_at, diag[h, :, pl.ds(at, span)].astype(F32), 0.0).astype(BF16)
        acc[h] = acc[h] + nt_dot(own.astype(BF16), corner)
    near = ((local, 0), (other, 0))
    for turn, places in zip(
        (0, *TURNS), (near, ((n1, 0), (n1, 16)), ((n2, 0), (n2, 16)), ((n3, 0), (n3, 16)))
    ):
        for core, (noise, row) in zip((mine, 1 - mine), places):
            number = 2 * lax.rem(chip + 4 - turn, 4) + core
            piece = noise[row : row + 16].astype(F32)
            piece = jnp.where(number < col, piece, 0.0).astype(BF16)
            from_ = pl.multiple_of(number * span, span)
            for h in range(2):
                acc[h] = acc[h] + nt_dot(piece, diag[h, :, pl.ds(from_, span)])
    for h in range(2):
        out[8 * h : 8 * h + 8] = acc[h][8 * h : 8 * h + 8]


def sample_kernel(mine, theirs, left, on_diag, out, samples):
    row, core = lax.axis_index(ROW), lax.axis_index("col_1")
    blocks = mine.shape[0]
    last = 8 * blocks - 1
    side = lax.broadcasted_iota(jnp.int32, (8, 256), 1) >> 6
    acc = on_diag[...]
    for half, coeffs in ((core, mine), (1 - core, theirs)):
        rows = []
        for i in range(blocks):
            slot = 4 * (half * blocks + i) + side
            c = coeffs[i].astype(F32)
            upper = jnp.where(slot < row, c, 0.0)
            lower = jnp.where((slot >= row) & (slot < last), c, 0.0)
            rows.append(jnp.concatenate([upper, lower], axis=0).astype(BF16))
        weights = jnp.concatenate(rows, axis=1)
        factor = left[pl.ds(half * blocks, blocks)].reshape(blocks * 256, left.shape[2])
        acc = acc + jnp.dot(weights, factor, preferred_element_type=F32)
    samples[...] = acc
    for n in range(out.shape[0]):
        out[n] = acc.astype(BF16)


def pack(table, words):
    tiles = [
        [table[p, 8 * h : 8 * h + 8].astype(F32) for h in range(2)] for p in range(table.shape[0])
    ]
    top = jnp.abs(tiles[0][0])
    for pair in tiles:
        for tile in pair:
            top = jnp.maximum(top, jnp.abs(tile))
    top = jnp.maximum(jnp.max(top, axis=1, keepdims=True), 1e-30)
    scale = 32700.0 / top
    for p, pair in enumerate(tiles):
        upper, lower = (jnp.round(tile * scale).astype(jnp.int32) for tile in pair)
        words[p] = (upper << 16) | (lower & 0xFFFF)
    return jnp.broadcast_to(top * (1.0 / 32700.0), (8, 128))


def lookup(words, unit, idx):
    low = idx & 127
    bit = [((idx >> (7 + n)) & 1) == 1 for n in range(5)]

    def tree(level, number):
        if level < 0:
            piece, half = number >> 1, number & 1
            source = words[piece, :, 128 * half : 128 * half + 128]
            return jnp.take_along_axis(source, low, axis=1, mode="promise_in_bounds")
        return jnp.where(bit[level], tree(level - 1, number | (1 << level)), tree(level - 1, number))

    word = tree(3, 0)
    return (jnp.where(bit[4], word << 16, word) >> 16).astype(F32) * unit


def own_kernel(table, first, partner, out, words):
    unit = pack(table, words)

    def step(n, carry):
        at = pl.multiple_of(n * 128, 128)
        a = jnp.broadcast_to(first[:, pl.ds(at, 128)], (8, 128))
        b = jnp.broadcast_to(partner[:, pl.ds(at, 128)], (8, 128))
        other = jnp.where(b >= 4096, lookup(words, unit, b), 0.0)
        out[:, pl.ds(at, 128)] = lookup(words, unit, a) - other
        return carry

    lax.fori_loop(0, first.shape[1] // 128, step, 0, unroll=16)


def emit_kernel(samples, out):
    for h in range(2):
        for s in range(8):
            out[s, h] = samples[8 * h + s : 8 * h + s + 1]


def put_rows(out, rows):
    for n in range(out.shape[0]):
        for i in range(9):
            out[n, :, 128 * i : 128 * i + 128] = rows[i]


def bin_kernel(prev, partner, base, onehot, counts, out, words, pieces):
    unit = pack(prev, words)

    def step(n, carry):
        at = pl.multiple_of(n * 128, 128)
        b = jnp.broadcast_to(partner[:, pl.ds(at, 128)], (8, 128))
        differ = base[:, pl.ds(at, 128)] - jnp.where(b < 4096, lookup(words, unit, b), 0.0)
        value = 0.5 * differ * differ
        top = value.astype(BF16).astype(F32)
        pieces[:, pl.ds(at, 128)] = jnp.concatenate([top, value - top], axis=0).astype(BF16)
        return carry

    lax.fori_loop(0, partner.shape[1] // 128, step, 0, unroll=16)
    total = nt_dot(pieces[...], onehot[...])
    sums = total[:8] + total[8:]
    put_rows(out, [sums[i : i + 1] for i in range(8)] + [counts[:1]])


def added(parts):
    total = parts[0]
    for n in range(1, parts.shape[0]):
        total = total + parts[n]
    return [total[:, 128 * i : 128 * i + 128] for i in range(9)]


def merge_kernel(parts, out):
    put_rows(out, added(parts))


def finish_kernel(parts, out):
    rows = added(parts)
    out[...] = jnp.concatenate(rows[:8], axis=0) / jnp.maximum(rows[8], 1.0)


def vmem(shape, dtype):
    return pltpu.VMEM(shape, dtype)


def body(
    noise, diag_factor, left_factor, right_factor, tile_ranks, pair_first, pair_partner, bin_ids
):
    rows = lax.axis_size(ROW)
    cols = lax.axis_size(COL)
    span = noise.shape[3]
    swap = [(0, 1), (1, 0)]
    first, partner, bins = pair_first[0], pair_partner[0], bin_ids[0]
    pairs = first.shape[1]

    local, spread_noise = call(
        copies_kernel,
        (
            vmem((16, span), BF16),
            vmem((rows, 16, span), BF16),
        ),
        [HB],
        flops=1 << 30,
        scratch_shapes=[pltpu.VMEM((8, 2, span), BF16), pltpu.SemaphoreType.DMA(())],
        name="copies",
    )(jnp.transpose(noise, (0, 2, 1, 3))[:, 0])
    columns = exchange(spread_noise, ROW)
    onehot, allowed, counts = call(
        prepare_kernel,
        (vmem((NBIN, pairs), BF16), vmem((8, 1, 256), F32), vmem((8, NBIN), F32)),
        [VM, SM],
        flops=1 << 20,
        name="prepare",
    )(bins, tile_ranks)
    other_noise = lax.ppermute(local, "col_1", swap)

    def project(away, name):
        return call(
            functools.partial(project_kernel, away=away),
            vmem((8, 8, 256), F32),
            [VM, VM],
            flops=1 << 28,
            name=name,
        )(columns, right_factor[0])

    send = project(True, "send")
    received = lax.ppermute(send, "col_1", swap)
    keep = project(False, "keep")
    payload = call(payload_kernel, vmem((96, span), F32), [VM] * 4, name="payload")(
        keep, received, local, other_noise
    ).astype(F16)
    arrived = []
    for turn in TURNS:
        arrived.append(
            lax.ppermute(payload, "col_0", [(chip, (chip + turn) % 4) for chip in range(4)])
        )
    total = sum(x[:64].astype(F32) for x in arrived).reshape(8, 8, span) * (1.0 / SUM_UNIT)
    total = (total + keep) + received
    mine = jnp.where(allowed > 0.5, total, 0.0).astype(BF16)
    all_noise = [
        (x[64:].astype(F32) * (1.0 / NOISE_UNIT)).astype(BF16) for x in arrived
    ]
    theirs = lax.ppermute(mine, "col_1", swap)
    on_diag = call(
        on_diag_kernel, vmem((16, span), F32), [VM] * 6, flops=1 << 28, name="ondiag"
    )(local, other_noise, *all_noise, diag_factor[:, 0])
    copies, own_samples = call(
        sample_kernel,
        (vmem((cols, 16, span), BF16), vmem((16, span), F32)),
        [VM, VM, VM, VM],
        flops=1 << 26,
        name="samples",
    )(mine, theirs, left_factor[0].reshape(16, 256, span), on_diag)
    own_tiles = exchange(copies, COL)
    prev_tiles = lax.ppermute(own_tiles, ROW, [(source, source + 1) for source in range(rows - 1)])
    samples = call(
        emit_kernel, jax.ShapeDtypeStruct((8, 2, 1, span), F32), [VM], name="emit"
    )(own_samples)
    base = call(
        own_kernel,
        vmem((8, pairs), F32),
        [VM, VM, VM],
        flops=1 << 26,
        scratch_shapes=[pltpu.VMEM((cols, 8, span), jnp.int32)],
        name="own",
    )(own_tiles, first, partner)
    partial = call(
        bin_kernel,
        vmem((lax.axis_size(ZC), 1, 9 * NBIN), F32),
        [VM, VM, VM, VM, VM],
        flops=1 << 26,
        scratch_shapes=[
            pltpu.VMEM((cols, 8, span), jnp.int32),
            pltpu.VMEM((16, pairs), BF16),
        ],
        name="bins",
    )(prev_tiles, partner, base, onehot, counts)
    merged = call(merge_kernel, vmem((lax.axis_size(XY), 1, 9 * NBIN), F32), [VM], name="merge")(
        exchange(partial, ZC)
    )
    variogram = call(finish_kernel, jax.ShapeDtypeStruct((8, NBIN), F32), [VM], name="finish")(exchange(merged, XY))
    return (samples, variogram)


def solution(mesh):
    split = Mesh(mesh.devices.reshape(4, 2, 4, 4, 2), ("row_0", "row_1", "row_2", "col_0", "col_1"))
    return jax.shard_map(
        body,
        mesh=split,
        in_specs=(
            P(None, None, ROW, COL),
            P(None, ROW, COL, None),
            P(ROW, None, None, COL),
            P(ROW, None, None, COL),
            P(ROW, None),
            P(ROW, COL, None),
            P(ROW, COL, None),
            P(ROW, COL, None),
        ),
        out_specs=(P(None, None, ROW, COL), P()),
        check_vma=False,
    )
```

```python
import functools

import jax
import jax.numpy as jnp
from jax import lax
from jax.experimental import pallas as pl
from jax.experimental.pallas import tpu as pltpu
from jax.sharding import Mesh
from jax.sharding import PartitionSpec as P

NBIN = 128
ROW = ("row_0", "row_1", "row_2")
COL = ("col_0", "col_1")
XY = ("row_0", "row_2")
ZC = ("row_1", "col_0", "col_1")
F32 = jnp.float32
F16 = jnp.float16
SUM_UNIT = 128.0
NOISE_UNIT = 1024.0
TURNS = (2, 1, 3)
BF16 = jnp.bfloat16


def exchange(copies, axis):
    return lax.all_to_all(copies, axis, 0, 0, tiled=True)


def nt_dot(a, b):
    return lax.dot_general(a, b, (((1,), (1,)), ((), ())), preferred_element_type=F32)


HB = pl.BlockSpec(memory_space=pltpu.HBM)
VM = pl.BlockSpec(memory_space=pltpu.VMEM)
SM = pl.BlockSpec(memory_space=pltpu.SMEM)


def call(kernel, out_shape, in_specs, flops=1, **kw):
    run = pl.pallas_call(
        kernel,
        out_shape=out_shape,
        in_specs=in_specs,
        cost_estimate=pl.CostEstimate(flops=flops, bytes_accessed=1 << 20, transcendentals=0),
        compiler_params=pltpu.CompilerParams(vmem_limit_bytes=16 << 20),
        **kw,
    )

    def held(*args):
        return run(
            *(
                a if spec is SM else pltpu.with_memory_space_constraint(a, spec.memory_space)
                for a, spec in zip(args, in_specs)
            )
        )

    return held


def copies_kernel(source, local, out, noise, sem):
    copy = pltpu.make_async_copy(source, noise, sem)
    copy.start()
    copy.wait()
    rows = [noise[s].astype(F32)[h : h + 1] for h in range(2) for s in range(8)]
    mine = jnp.concatenate(rows, axis=0).astype(BF16)
    local[...] = mine
    for n in range(out.shape[0]):
        out[n] = mine


def prepare_kernel(bins, ranks, onehot, keep, counts):
    core = lax.axis_index("col_1")
    lane = lax.broadcasted_iota(jnp.int32, (1, 256), 1)
    for i in range(keep.shape[0]):
        slot = 4 * (core * keep.shape[0] + i)
        limit = ranks[0, slot + 3] + 192
        for n in (2, 1, 0):
            limit = jnp.where(lane < 64 * n + 64, ranks[0, slot + n] + 64 * n, limit)
        keep[i] = jnp.where(lane < limit, 1.0, 0.0)
    bin_at = lax.broadcasted_iota(jnp.int32, (NBIN, 128), 0)

    def step(n, carry):
        at = pl.multiple_of(n * 128, 128)
        ids = jnp.broadcast_to(bins[:, pl.ds(at, 128)], (NBIN, 128))
        onehot[:, pl.ds(at, 128)] = jnp.where(ids == bin_at, 1.0, 0.0).astype(BF16)
        return carry

    lax.fori_loop(0, bins.shape[1] // 128, step, 0, unroll=4)
    counts[...] = nt_dot(jnp.ones((8, onehot.shape[1]), BF16), onehot[...])


def payload_kernel(keep, received, local, other, out):
    for g in range(keep.shape[0]):
        out[8 * g : 8 * g + 8] = (keep[g] + received[g]) * SUM_UNIT
    out[64:80] = local[...].astype(F32) * NOISE_UNIT
    out[80:] = other[...].astype(F32) * NOISE_UNIT


def project_kernel(columns, right, out, *, away):
    row, core = lax.axis_index(ROW), lax.axis_index("col_1")
    half = 1 - core if away else core
    tiles = 2 * columns.shape[0]
    groups = out.shape[0]
    lane = lax.broadcasted_iota(jnp.int32, (8, 128), 1)

    def step(g, carry):
        base = (half * groups + g) * 4
        blocks = []
        low = []
        for n in range(4):
            slot = base + n
            tile = jnp.where(slot < row, slot, slot - row)
            first = tile < tiles // 2
            blocks.append(columns[jnp.where(first, tile, tiles - 1 - tile)])
            low.append(first)
        factor = right[pl.ds(base, 4)].reshape(256, 256)
        full = nt_dot(jnp.concatenate(blocks, axis=0), factor)
        parts = []
        for n in range(4):
            cols = full[16 * n : 16 * n + 16, 128 * (n // 2) : 128 * (n // 2) + 128]
            parts.append(jnp.where(low[n], cols[:8], cols[8:]))
        out[g, :, :128] = jnp.where(lane < 64, parts[0], parts[1])
        out[g, :, 128:] = jnp.where(lane < 64, parts[2], parts[3])
        return carry

    lax.fori_loop(0, groups, step, 0, unroll=4)


def on_diag_kernel(local, other, n1, n2, n3, diag, out):
    col, chip, mine = lax.axis_index(COL), lax.axis_index("col_0"), lax.axis_index("col_1")
    span = diag.shape[1]
    own = local[...].astype(F32)
    i_at = lax.broadcasted_iota(jnp.int32, (span, span), 0)
    j_at = lax.broadcasted_iota(jnp.int32, (span, span), 1)
    acc = [own, own]
    at = pl.multiple_of(col * span, span)
    for h in range(2):
        corner = jnp.where(j_at < i_at, diag[h, :, pl.ds(at, span)].astype(F32), 0.0).astype(BF16)
        acc[h] = acc[h] + nt_dot(own.astype(BF16), corner)
    near = ((local, 0), (other, 0))
    for turn, places in zip(
        (0, *TURNS), (near, ((n1, 0), (n1, 16)), ((n2, 0), (n2, 16)), ((n3, 0), (n3, 16)))
    ):
        for core, (noise, row) in zip((mine, 1 - mine), places):
            number = 2 * lax.rem(chip + 4 - turn, 4) + core
            piece = noise[row : row + 16].astype(F32)
            piece = jnp.where(number < col, piece, 0.0).astype(BF16)
            from_ = pl.multiple_of(number * span, span)
            for h in range(2):
                acc[h] = acc[h] + nt_dot(piece, diag[h, :, pl.ds(from_, span)])
    for h in range(2):
        out[8 * h : 8 * h + 8] = acc[h][8 * h : 8 * h + 8]


def sample_kernel(mine, theirs, left, on_diag, out, samples):
    row, core = lax.axis_index(ROW), lax.axis_index("col_1")
    blocks = mine.shape[0]
    last = 8 * blocks - 1
    side = lax.broadcasted_iota(jnp.int32, (8, 256), 1) >> 6
    acc = on_diag[...]
    for half, coeffs in ((core, mine), (1 - core, theirs)):
        rows = []
        for i in range(blocks):
            slot = 4 * (half * blocks + i) + side
            c = coeffs[i].astype(F32)
            upper = jnp.where(slot < row, c, 0.0)
            lower = jnp.where((slot >= row) & (slot < last), c, 0.0)
            rows.append(jnp.concatenate([upper, lower], axis=0).astype(BF16))
        weights = jnp.concatenate(rows, axis=1)
        factor = left[pl.ds(half * blocks, blocks)].reshape(blocks * 256, left.shape[2])
        acc = acc + jnp.dot(weights, factor, preferred_element_type=F32)
    samples[...] = acc
    out[...] = acc.astype(BF16)


def pack(mine, theirs, words):
    chip, core = lax.axis_index("col_0"), lax.axis_index("col_1")
    tiles, places = [], []
    for part, side in ((mine, core), (theirs, 1 - core)):
        for n, turn in enumerate((0, *TURNS)):
            tiles.append([part[n, 8 * h : 8 * h + 8].astype(F32) for h in range(2)])
            places.append(2 * lax.rem(chip + 4 - turn, 4) + side)
    top = jnp.abs(tiles[0][0])
    for pair in tiles:
        for tile in pair:
            top = jnp.maximum(top, jnp.abs(tile))
    top = jnp.maximum(jnp.max(top, axis=1, keepdims=True), 1e-30)
    scale = 32700.0 / top
    for place, pair in zip(places, tiles):
        upper, lower = (jnp.round(tile * scale).astype(jnp.int32) for tile in pair)
        words[place] = (upper << 16) | (lower & 0xFFFF)
    return jnp.broadcast_to(top * (1.0 / 32700.0), (8, 128))


def lookup(words, unit, idx):
    low = idx & 127
    bit = [((idx >> (7 + n)) & 1) == 1 for n in range(5)]

    def tree(level, number):
        if level < 0:
            piece, half = number >> 1, number & 1
            source = words[piece, :, 128 * half : 128 * half + 128]
            return jnp.take_along_axis(source, low, axis=1, mode="promise_in_bounds")
        return jnp.where(bit[level], tree(level - 1, number | (1 << level)), tree(level - 1, number))

    word = tree(3, 0)
    return (jnp.where(bit[4], word << 16, word) >> 16).astype(F32) * unit


def own_kernel(mine, theirs, first, partner, out, words):
    unit = pack(mine, theirs, words)

    def step(n, carry):
        at = pl.multiple_of(n * 128, 128)
        a = jnp.broadcast_to(first[:, pl.ds(at, 128)], (8, 128))
        b = jnp.broadcast_to(partner[:, pl.ds(at, 128)], (8, 128))
        other = jnp.where(b >= 4096, lookup(words, unit, b), 0.0)
        out[:, pl.ds(at, 128)] = lookup(words, unit, a) - other
        return carry

    lax.fori_loop(0, first.shape[1] // 128, step, 0, unroll=16)


def emit_kernel(samples, out):
    for h in range(2):
        for s in range(8):
            out[s, h] = samples[8 * h + s : 8 * h + s + 1]


def put_rows(out, rows):
    for n in range(out.shape[0]):
        for i in range(9):
            out[n, :, 128 * i : 128 * i + 128] = rows[i]


def bin_kernel(mine, theirs, partner, base, onehot, counts, out, words, pieces):
    unit = pack(mine, theirs, words)

    def step(n, carry):
        at = pl.multiple_of(n * 128, 128)
        b = jnp.broadcast_to(partner[:, pl.ds(at, 128)], (8, 128))
        differ = base[:, pl.ds(at, 128)] - jnp.where(b < 4096, lookup(words, unit, b), 0.0)
        value = 0.5 * differ * differ
        top = value.astype(BF16).astype(F32)
        pieces[:, pl.ds(at, 128)] = jnp.concatenate([top, value - top], axis=0).astype(BF16)
        return carry

    lax.fori_loop(0, partner.shape[1] // 128, step, 0, unroll=16)
    total = nt_dot(pieces[...], onehot[...])
    sums = total[:8] + total[8:]
    put_rows(out, [sums[i : i + 1] for i in range(8)] + [counts[:1]])


def added(parts):
    total = parts[0]
    for n in range(1, parts.shape[0]):
        total = total + parts[n]
    return [total[:, 128 * i : 128 * i + 128] for i in range(9)]


def merge_kernel(parts, out):
    put_rows(out, added(parts))


def finish_kernel(parts, out):
    rows = added(parts)
    out[...] = jnp.concatenate(rows[:8], axis=0) / jnp.maximum(rows[8], 1.0)


def vmem(shape, dtype):
    return pltpu.VMEM(shape, dtype)


def body(
    noise, diag_factor, left_factor, right_factor, tile_ranks, pair_first, pair_partner, bin_ids
):
    rows = lax.axis_size(ROW)
    cols = lax.axis_size(COL)
    span = noise.shape[3]
    swap = [(0, 1), (1, 0)]
    first, partner, bins = pair_first[0], pair_partner[0], bin_ids[0]
    pairs = first.shape[1]

    local, spread_noise = call(
        copies_kernel,
        (
            vmem((16, span), BF16),
            vmem((rows, 16, span), BF16),
        ),
        [HB],
        flops=1 << 30,
        scratch_shapes=[pltpu.VMEM((8, 2, span), BF16), pltpu.SemaphoreType.DMA(())],
        name="copies",
    )(jnp.transpose(noise, (0, 2, 1, 3))[:, 0])
    columns = exchange(spread_noise, ROW)
    onehot, allowed, counts = call(
        prepare_kernel,
        (vmem((NBIN, pairs), BF16), vmem((8, 1, 256), F32), vmem((8, NBIN), F32)),
        [VM, SM],
        flops=1 << 20,
        name="prepare",
    )(bins, tile_ranks)
    other_noise = lax.ppermute(local, "col_1", swap)

    def project(away, name):
        return call(
            functools.partial(project_kernel, away=away),
            vmem((8, 8, 256), F32),
            [VM, VM],
            flops=1 << 28,
            name=name,
        )(columns, right_factor[0])

    send = project(True, "send")
    received = lax.ppermute(send, "col_1", swap)
    keep = project(False, "keep")
    payload = call(payload_kernel, vmem((96, span), F32), [VM] * 4, name="payload")(
        keep, received, local, other_noise
    ).astype(F16)
    arrived = []
    for turn in TURNS:
        arrived.append(
            lax.ppermute(payload, "col_0", [(chip, (chip + turn) % 4) for chip in range(4)])
        )
    total = sum(x[:64].astype(F32) for x in arrived).reshape(8, 8, span) * (1.0 / SUM_UNIT)
    total = (total + keep) + received
    mine = jnp.where(allowed > 0.5, total, 0.0).astype(BF16)
    all_noise = [
        (x[64:].astype(F32) * (1.0 / NOISE_UNIT)).astype(BF16) for x in arrived
    ]
    theirs = lax.ppermute(mine, "col_1", swap)
    on_diag = call(
        on_diag_kernel, vmem((16, span), F32), [VM] * 6, flops=1 << 28, name="ondiag"
    )(local, other_noise, *all_noise, diag_factor[:, 0])
    piece, own_samples = call(
        sample_kernel,
        (vmem((16, span), BF16), vmem((16, span), F32)),
        [VM, VM, VM, VM],
        flops=1 << 26,
        name="samples",
    )(mine, theirs, left_factor[0].reshape(16, 256, span), on_diag)
    pieces = [piece]
    for turn in TURNS:
        pieces.append(
            lax.ppermute(piece, "col_0", [(chip, (chip + turn) % 4) for chip in range(4)])
        )
    own_mine = jnp.stack(pieces)
    prev_mine = lax.ppermute(own_mine, ROW, [(source, source + 1) for source in range(rows - 1)])
    own_theirs = lax.ppermute(own_mine, "col_1", swap)
    prev_theirs = lax.ppermute(prev_mine, "col_1", swap)
    samples = call(
        emit_kernel, jax.ShapeDtypeStruct((8, 2, 1, span), F32), [VM], name="emit"
    )(own_samples)
    base = call(
        own_kernel,
        vmem((8, pairs), F32),
        [VM] * 4,
        flops=1 << 26,
        scratch_shapes=[pltpu.VMEM((cols, 8, span), jnp.int32)],
        name="own",
    )(own_mine, own_theirs, first, partner)
    partial = call(
        bin_kernel,
        vmem((lax.axis_size(ZC), 1, 9 * NBIN), F32),
        [VM] * 6,
        flops=1 << 26,
        scratch_shapes=[
            pltpu.VMEM((cols, 8, span), jnp.int32),
            pltpu.VMEM((16, pairs), BF16),
        ],
        name="bins",
    )(prev_mine, prev_theirs, partner, base, onehot, counts)
    merged = call(merge_kernel, vmem((lax.axis_size(XY), 1, 9 * NBIN), F32), [VM], name="merge")(
        exchange(partial, ZC)
    )
    variogram = call(finish_kernel, jax.ShapeDtypeStruct((8, NBIN), F32), [VM], name="finish")(exchange(merged, XY))
    return (samples, variogram)


def solution(mesh):
    split = Mesh(mesh.devices.reshape(4, 2, 4, 4, 2), ("row_0", "row_1", "row_2", "col_0", "col_1"))
    return jax.shard_map(
        body,
        mesh=split,
        in_specs=(
            P(None, None, ROW, COL),
            P(None, ROW, COL, None),
            P(ROW, None, None, COL),
            P(ROW, None, None, COL),
            P(ROW, None),
            P(ROW, COL, None),
            P(ROW, COL, None),
            P(ROW, COL, None),
        ),
        out_specs=(P(None, None, ROW, COL), P()),
        check_vma=False,
    )
```

```python
import functools

import jax
import jax.numpy as jnp
from jax import lax
from jax.experimental import pallas as pl
from jax.experimental.pallas import tpu as pltpu
from jax.sharding import Mesh
from jax.sharding import PartitionSpec as P

NBIN = 128
ROW = ("row_0", "row_1", "row_2")
COL = ("col_0", "col_1")
XY = ("row_0", "row_2")
ZC = ("row_1", "col_0", "col_1")
F32 = jnp.float32
F16 = jnp.float16
SUM_UNIT = 128.0
NOISE_UNIT = 1024.0
TURNS = (2, 1, 3)
BF16 = jnp.bfloat16


def exchange(copies, axis):
    return lax.all_to_all(copies, axis, 0, 0, tiled=True)


def nt_dot(a, b):
    return lax.dot_general(a, b, (((1,), (1,)), ((), ())), preferred_element_type=F32)


HB = pl.BlockSpec(memory_space=pltpu.HBM)
VM = pl.BlockSpec(memory_space=pltpu.VMEM)
SM = pl.BlockSpec(memory_space=pltpu.SMEM)


def call(kernel, out_shape, in_specs, flops=1, **kw):
    run = pl.pallas_call(
        kernel,
        out_shape=out_shape,
        in_specs=in_specs,
        cost_estimate=pl.CostEstimate(flops=flops, bytes_accessed=1 << 20, transcendentals=0),
        compiler_params=pltpu.CompilerParams(vmem_limit_bytes=16 << 20),
        **kw,
    )

    def held(*args):
        return run(
            *(
                a if spec is SM else pltpu.with_memory_space_constraint(a, spec.memory_space)
                for a, spec in zip(args, in_specs)
            )
        )

    return held


def copies_kernel(source, local, out, noise, sem):
    copy = pltpu.make_async_copy(source, noise, sem)
    copy.start()
    copy.wait()
    rows = [noise[s].astype(F32)[h : h + 1] for h in range(2) for s in range(8)]
    mine = jnp.concatenate(rows, axis=0).astype(BF16)
    local[...] = mine
    for n in range(out.shape[0]):
        out[n] = mine


def mask_kernel(ranks, keep):
    core = lax.axis_index("col_1")
    lane = lax.broadcasted_iota(jnp.int32, (1, 256), 1)
    for i in range(keep.shape[0]):
        slot = 4 * (core * keep.shape[0] + i)
        limit = ranks[0, slot + 3] + 192
        for n in (2, 1, 0):
            limit = jnp.where(lane < 64 * n + 64, ranks[0, slot + n] + 64 * n, limit)
        keep[i] = jnp.where(lane < limit, 1.0, 0.0)


def prepare_kernel(bins, onehot, counts):
    bin_at = lax.broadcasted_iota(jnp.int32, (NBIN, 128), 0)

    def step(n, carry):
        at = pl.multiple_of(n * 128, 128)
        ids = jnp.broadcast_to(bins[:, pl.ds(at, 128)], (NBIN, 128))
        onehot[:, pl.ds(at, 128)] = jnp.where(ids == bin_at, 1.0, 0.0).astype(BF16)
        return carry

    lax.fori_loop(0, bins.shape[1] // 128, step, 0, unroll=4)
    counts[...] = nt_dot(jnp.ones((8, onehot.shape[1]), BF16), onehot[...])


def payload_kernel(keep, received, local, other, out):
    for g in range(keep.shape[0]):
        out[8 * g : 8 * g + 8] = (keep[g] + received[g]) * SUM_UNIT
    out[64:80] = local[...].astype(F32) * NOISE_UNIT
    out[80:] = other[...].astype(F32) * NOISE_UNIT


def project_kernel(columns, right, out, *, away):
    row, core = lax.axis_index(ROW), lax.axis_index("col_1")
    half = 1 - core if away else core
    tiles = 2 * columns.shape[0]
    groups = out.shape[0]
    lane = lax.broadcasted_iota(jnp.int32, (8, 128), 1)

    def step(g, carry):
        base = (half * groups + g) * 4
        blocks = []
        low = []
        for n in range(4):
            slot = base + n
            tile = jnp.where(slot < row, slot, slot - row)
            first = tile < tiles // 2
            blocks.append(columns[jnp.where(first, tile, tiles - 1 - tile)])
            low.append(first)
        factor = right[pl.ds(base, 4)].reshape(256, 256)
        full = nt_dot(jnp.concatenate(blocks, axis=0), factor)
        parts = []
        for n in range(4):
            cols = full[16 * n : 16 * n + 16, 128 * (n // 2) : 128 * (n // 2) + 128]
            parts.append(jnp.where(low[n], cols[:8], cols[8:]))
        out[g, :, :128] = jnp.where(lane < 64, parts[0], parts[1])
        out[g, :, 128:] = jnp.where(lane < 64, parts[2], parts[3])
        return carry

    lax.fori_loop(0, groups, step, 0, unroll=4)


def on_diag_kernel(local, other, n1, n2, n3, diag, out):
    col, chip, mine = lax.axis_index(COL), lax.axis_index("col_0"), lax.axis_index("col_1")
    span = diag.shape[1]
    own = local[...].astype(F32)
    i_at = lax.broadcasted_iota(jnp.int32, (span, span), 0)
    j_at = lax.broadcasted_iota(jnp.int32, (span, span), 1)
    acc = [own, own]
    at = pl.multiple_of(col * span, span)
    for h in range(2):
        corner = jnp.where(j_at < i_at, diag[h, :, pl.ds(at, span)].astype(F32), 0.0).astype(BF16)
        acc[h] = acc[h] + nt_dot(own.astype(BF16), corner)
    near = ((local, 0), (other, 0))
    for turn, places in zip(
        (0, *TURNS), (near, ((n1, 0), (n1, 16)), ((n2, 0), (n2, 16)), ((n3, 0), (n3, 16)))
    ):
        for core, (noise, row) in zip((mine, 1 - mine), places):
            number = 2 * lax.rem(chip + 4 - turn, 4) + core
            piece = noise[row : row + 16].astype(F32)
            piece = jnp.where(number < col, piece, 0.0).astype(BF16)
            from_ = pl.multiple_of(number * span, span)
            for h in range(2):
                acc[h] = acc[h] + nt_dot(piece, diag[h, :, pl.ds(from_, span)])
    for h in range(2):
        out[8 * h : 8 * h + 8] = acc[h][8 * h : 8 * h + 8]


def sample_kernel(mine, theirs, left, on_diag, out, samples):
    row, core = lax.axis_index(ROW), lax.axis_index("col_1")
    blocks = mine.shape[0]
    last = 8 * blocks - 1
    side = lax.broadcasted_iota(jnp.int32, (8, 256), 1) >> 6
    acc = on_diag[...]
    for half, coeffs in ((core, mine), (1 - core, theirs)):
        rows = []
        for i in range(blocks):
            slot = 4 * (half * blocks + i) + side
            c = coeffs[i].astype(F32)
            upper = jnp.where(slot < row, c, 0.0)
            lower = jnp.where((slot >= row) & (slot < last), c, 0.0)
            rows.append(jnp.concatenate([upper, lower], axis=0).astype(BF16))
        weights = jnp.concatenate(rows, axis=1)
        factor = left[pl.ds(half * blocks, blocks)].reshape(blocks * 256, left.shape[2])
        acc = acc + jnp.dot(weights, factor, preferred_element_type=F32)
    samples[...] = acc
    out[...] = acc.astype(BF16)


def pack(mine, theirs, words):
    chip, core = lax.axis_index("col_0"), lax.axis_index("col_1")
    tiles, places = [], []
    for part, side in ((mine, core), (theirs, 1 - core)):
        for n, turn in enumerate((0, *TURNS)):
            tiles.append([part[n, 8 * h : 8 * h + 8].astype(F32) for h in range(2)])
            places.append(2 * lax.rem(chip + 4 - turn, 4) + side)
    top = jnp.abs(tiles[0][0])
    for pair in tiles:
        for tile in pair:
            top = jnp.maximum(top, jnp.abs(tile))
    top = jnp.maximum(jnp.max(top, axis=1, keepdims=True), 1e-30)
    scale = 32700.0 / top
    for place, pair in zip(places, tiles):
        upper, lower = (jnp.round(tile * scale).astype(jnp.int32) for tile in pair)
        words[place] = (upper << 16) | (lower & 0xFFFF)
    return jnp.broadcast_to(top * (1.0 / 32700.0), (8, 128))


def lookup(words, unit, idx):
    low = idx & 127
    bit = [((idx >> (7 + n)) & 1) == 1 for n in range(5)]

    def tree(level, number):
        if level < 0:
            piece, half = number >> 1, number & 1
            source = words[piece, :, 128 * half : 128 * half + 128]
            return jnp.take_along_axis(source, low, axis=1, mode="promise_in_bounds")
        return jnp.where(bit[level], tree(level - 1, number | (1 << level)), tree(level - 1, number))

    word = tree(3, 0)
    return (jnp.where(bit[4], word << 16, word) >> 16).astype(F32) * unit


def own_kernel(mine, theirs, first, partner, out, words):
    unit = pack(mine, theirs, words)

    def step(n, carry):
        at = pl.multiple_of(n * 128, 128)
        a = jnp.broadcast_to(first[:, pl.ds(at, 128)], (8, 128))
        b = jnp.broadcast_to(partner[:, pl.ds(at, 128)], (8, 128))
        other = jnp.where(b >= 4096, lookup(words, unit, b), 0.0)
        out[:, pl.ds(at, 128)] = lookup(words, unit, a) - other
        return carry

    lax.fori_loop(0, first.shape[1] // 128, step, 0, unroll=16)


def emit_kernel(samples, out):
    for h in range(2):
        for s in range(8):
            out[s, h] = samples[8 * h + s : 8 * h + s + 1]


def put_rows(out, rows):
    for n in range(out.shape[0]):
        for i in range(9):
            out[n, :, 128 * i : 128 * i + 128] = rows[i]


def bin_kernel(mine, theirs, partner, base, onehot, counts, out, words, pieces):
    unit = pack(mine, theirs, words)

    def step(n, carry):
        at = pl.multiple_of(n * 128, 128)
        b = jnp.broadcast_to(partner[:, pl.ds(at, 128)], (8, 128))
        differ = base[:, pl.ds(at, 128)] - jnp.where(b < 4096, lookup(words, unit, b), 0.0)
        value = 0.5 * differ * differ
        top = value.astype(BF16).astype(F32)
        pieces[:, pl.ds(at, 128)] = jnp.concatenate([top, value - top], axis=0).astype(BF16)
        return carry

    lax.fori_loop(0, partner.shape[1] // 128, step, 0, unroll=16)
    total = nt_dot(pieces[...], onehot[...])
    sums = total[:8] + total[8:]
    put_rows(out, [sums[i : i + 1] for i in range(8)] + [counts[:1]])


def added(parts):
    total = parts[0]
    for n in range(1, parts.shape[0]):
        total = total + parts[n]
    return [total[:, 128 * i : 128 * i + 128] for i in range(9)]


def merge_kernel(parts, out):
    put_rows(out, added(parts))


def finish_kernel(parts, out):
    rows = added(parts)
    out[...] = jnp.concatenate(rows[:8], axis=0) / jnp.maximum(rows[8], 1.0)


def vmem(shape, dtype):
    return pltpu.VMEM(shape, dtype)


def body(
    noise, diag_factor, left_factor, right_factor, tile_ranks, pair_first, pair_partner, bin_ids
):
    rows = lax.axis_size(ROW)
    cols = lax.axis_size(COL)
    span = noise.shape[3]
    swap = [(0, 1), (1, 0)]
    first, partner, bins = pair_first[0], pair_partner[0], bin_ids[0]
    pairs = first.shape[1]

    local, spread_noise = call(
        copies_kernel,
        (
            vmem((16, span), BF16),
            vmem((rows, 16, span), BF16),
        ),
        [HB],
        flops=1 << 30,
        scratch_shapes=[pltpu.VMEM((8, 2, span), BF16), pltpu.SemaphoreType.DMA(())],
        name="copies",
    )(jnp.transpose(noise, (0, 2, 1, 3))[:, 0])
    columns = exchange(spread_noise, ROW)
    allowed = call(mask_kernel, vmem((8, 1, 256), F32), [SM], name="mask")(tile_ranks)
    onehot, counts = call(
        prepare_kernel,
        (vmem((NBIN, pairs), BF16), vmem((8, NBIN), F32)),
        [VM],
        flops=1 << 20,
        name="prepare",
    )(bins)
    other_noise = lax.ppermute(local, "col_1", swap)

    def project(away, name):
        return call(
            functools.partial(project_kernel, away=away),
            vmem((8, 8, 256), F32),
            [VM, VM],
            flops=1 << 28,
            name=name,
        )(columns, right_factor[0])

    send = project(True, "send")
    received = lax.ppermute(send, "col_1", swap)
    keep = project(False, "keep")
    payload = call(payload_kernel, vmem((96, span), F32), [VM] * 4, name="payload")(
        keep, received, local, other_noise
    ).astype(F16)
    arrived = []
    for turn in TURNS:
        arrived.append(
            lax.ppermute(payload, "col_0", [(chip, (chip + turn) % 4) for chip in range(4)])
        )
    total = sum(x[:64].astype(F32) for x in arrived).reshape(8, 8, span) * (1.0 / SUM_UNIT)
    total = (total + keep) + received
    mine = jnp.where(allowed > 0.5, total, 0.0).astype(BF16)
    all_noise = [
        (x[64:].astype(F32) * (1.0 / NOISE_UNIT)).astype(BF16) for x in arrived
    ]
    theirs = lax.ppermute(mine, "col_1", swap)
    on_diag = call(
        on_diag_kernel, vmem((16, span), F32), [VM] * 6, flops=1 << 28, name="ondiag"
    )(local, other_noise, *all_noise, diag_factor[:, 0])
    piece, own_samples = call(
        sample_kernel,
        (vmem((16, span), BF16), vmem((16, span), F32)),
        [VM, VM, VM, VM],
        flops=1 << 26,
        name="samples",
    )(mine, theirs, left_factor[0].reshape(16, 256, span), on_diag)
    pieces = [piece]
    for turn in TURNS:
        pieces.append(
            lax.ppermute(piece, "col_0", [(chip, (chip + turn) % 4) for chip in range(4)])
        )
    own_mine = jnp.stack(pieces)
    prev_mine = lax.ppermute(own_mine, ROW, [(source, source + 1) for source in range(rows - 1)])
    own_theirs = lax.ppermute(own_mine, "col_1", swap)
    prev_theirs = lax.ppermute(prev_mine, "col_1", swap)
    samples = call(
        emit_kernel, jax.ShapeDtypeStruct((8, 2, 1, span), F32), [VM], name="emit"
    )(own_samples)
    base = call(
        own_kernel,
        vmem((8, pairs), F32),
        [VM] * 4,
        flops=1 << 26,
        scratch_shapes=[pltpu.VMEM((cols, 8, span), jnp.int32)],
        name="own",
    )(own_mine, own_theirs, first, partner)
    partial = call(
        bin_kernel,
        vmem((lax.axis_size(ZC), 1, 9 * NBIN), F32),
        [VM] * 6,
        flops=1 << 26,
        scratch_shapes=[
            pltpu.VMEM((cols, 8, span), jnp.int32),
            pltpu.VMEM((16, pairs), BF16),
        ],
        name="bins",
    )(prev_mine, prev_theirs, partner, base, onehot, counts)
    merged = call(merge_kernel, vmem((lax.axis_size(XY), 1, 9 * NBIN), F32), [VM], name="merge")(
        exchange(partial, ZC)
    )
    variogram = call(finish_kernel, jax.ShapeDtypeStruct((8, NBIN), F32), [VM], name="finish")(exchange(merged, XY))
    return (samples, variogram)


def solution(mesh):
    split = Mesh(mesh.devices.reshape(4, 2, 4, 4, 2), ("row_0", "row_1", "row_2", "col_0", "col_1"))
    return jax.shard_map(
        body,
        mesh=split,
        in_specs=(
            P(None, None, ROW, COL),
            P(None, ROW, COL, None),
            P(ROW, None, None, COL),
            P(ROW, None, None, COL),
            P(ROW, None),
            P(ROW, COL, None),
            P(ROW, COL, None),
            P(ROW, COL, None),
        ),
        out_specs=(P(None, None, ROW, COL), P()),
        check_vma=False,
    )
```
